32 devices in a mesh: fsdp: 32 (over z, y, x, core).
Axes of the slice: x: 2, y: 2, z: 4, core: 2. Of those that a mesh axis runs over, the one named last changes fastest.
Arguments:
- images: bfloat16 [2, 64, 197, 384], P(None, 'fsdp'), may hold values from -6 to 6
- cotangent: bfloat16 [2, 64, 197, 384], P(None, 'fsdp'), may hold values from -6 to 6
- counts: int32 [2, 32], P(None, 'fsdp'), may hold values from 1 to 2, as said below
- master: float32 [2, 1777664], P(None, 'fsdp'), may hold values from -10 to 10, as said below
- moment_one: float32 [2, 1777664], P(None, 'fsdp'), may hold values from -0.3125 to 0.3125
- moment_two: float32 [2, 1777664], P(None, 'fsdp'), may hold values from 1e-06 to 0.0001
Outputs:
- activations: bfloat16 [2, 64, 197, 384], P(None, 'fsdp')
- input_grad: float32 [2, 64, 197, 384], P(None, 'fsdp')
- weight_grad: float32 [2, 1777664], P(None, 'fsdp')
- new_master: float32 [2, 1777664], P(None, 'fsdp')
- new_moment_one: float32 [2, 1777664], P(None, 'fsdp')
- new_moment_two: float32 [2, 1777664], P(None, 'fsdp')
The draws below stay inside these ranges and needn't reach their ends.
Inputs may be any that keep to these rules, and one draw needn't show every extreme that they name: `counts`: each device has one or two live slots in every micro-batch; in every micro-batch some device has two and some has one. `master`: gains lie near one; biases and matrix entries are bounded.
All inputs are finite; a program needn't handle non-finite values.
Results may differ from the reference program's by a relative error of at most 0.017.
Values may be sent and summed in bfloat16 or wider, within the bound.
A program may use at most 256 MiB of HBM per device.

```python
import math
import jax
import jax.numpy as jnp
from jax import lax

D = 384
H = 6
HD = 64
FF = 1536
SEQ = 197
LAYERS = 2
SLOTS = 2
MICRO = 2
STEP = 3
IMAGES = 128
NPAR = 1774080
NPAD = 1777664
N_FSDP = 32


def draw_counts(key, part):
    base = jax.random.randint(jax.random.fold_in(key, 1), (MICRO, N_FSDP), 1, 3)
    orders = jax.vmap(lambda sub: jax.random.permutation(sub, N_FSDP))(jax.random.split(jax.random.fold_in(key, 2), MICRO))
    columns = jnp.arange(N_FSDP)[None, :]
    full_slot = columns == orders[:, 0:1]
    single_slot = columns == orders[:, 1:2]
    return jnp.where(full_slot, 2, jnp.where(single_slot, 1, base)).astype(jnp.int32)


def layer_params(key):
    keys = jax.random.split(key, 13)

    def gain_draw(sub, count):
        return 1.0 + 0.2 * jax.random.uniform(sub, (count,), jnp.float32, -1.0, 1.0)

    def shift_draw(sub, count, scale):
        return jnp.clip(scale * jax.random.normal(sub, (count,), jnp.float32), -4.0, 4.0)

    def matrix_draw(sub, height, breadth, scale):
        return jnp.clip(jax.random.normal(sub, (height, breadth), jnp.float32), -5.0, 5.0) * scale
    qkv_weight = matrix_draw(keys[9], D, 3 * D, D ** (-0.5))
    pieces = [gain_draw(keys[0], D), shift_draw(keys[1], D, 0.3), shift_draw(keys[2], D, 0.5), shift_draw(keys[3], D, 0.5), shift_draw(keys[4], D, 0.3), gain_draw(keys[5], D), shift_draw(keys[6], D, 0.3), shift_draw(keys[7], D, 0.3), shift_draw(keys[8], FF, 0.5), qkv_weight.reshape(-1), matrix_draw(keys[10], D, D, 2.0 * D ** (-0.5)).reshape(-1), matrix_draw(keys[11], D, FF, D ** (-0.5)).reshape(-1), matrix_draw(keys[12], FF, D, FF ** (-0.5)).reshape(-1)]
    filler = 0.02 * jax.random.normal(jax.random.fold_in(key, 99), (NPAD - NPAR,), jnp.float32)
    return jnp.concatenate(pieces + [filler])


def draw_master(key, part):
    return jnp.stack([layer_params(jax.random.fold_in(key, 10 + index)) for index in range(LAYERS)])


def block_levels(key, dims, shards, least, top_value):
    level, own = 1.0, jax.random.fold_in(key, 6)
    for position, parts in shards:
        steps = jnp.exp(jax.random.uniform(jax.random.fold_in(own, position), (parts,), jnp.float32, least / len(shards), top_value / len(shards)))
        level = level * jnp.repeat(steps, dims[position] // parts).reshape([-1 if axis == position else 1 for axis in range(len(dims))])
    return level


def noise(stream_key, shape, scale, reach, cuts=(), kind=jnp.bfloat16):
    level = block_levels(stream_key, shape, cuts, -0.22, 0.18) if cuts else 1.0
    drawn = jax.random.normal(stream_key, shape, jnp.float32) * scale * level
    return jnp.minimum(jnp.maximum(drawn, -reach), reach).astype(kind)


def setup_inputs(seed: int = 0) -> dict:
    splits = jax.random.split(jax.random.key(seed), 7)
    images = noise(splits[0], (MICRO, SLOTS * N_FSDP, SEQ, D), 1.0, 6.0, ((1, 32),))
    cotangent = noise(splits[1], (MICRO, SLOTS * N_FSDP, SEQ, D), 1.0, 6.0, ((1, 32),))
    counts = draw_counts(jax.random.fold_in(splits[6], 71), 0)
    master = draw_master(jax.random.fold_in(splits[6], 71), 0)
    moment_one = noise(splits[4], (LAYERS, NPAD), 0.02, 0.3125, ((1, 32),), jnp.float32)
    moment_two = jnp.clip(jnp.exp(math.log(0.0001) - 4.6051702 * jax.random.uniform(splits[5], (LAYERS, NPAD), jnp.float32) ** block_levels(splits[5], (LAYERS, NPAD), ((1, 32),), -0.2, 0.2)), 9.999999974752427e-07, 0.0001)
    return {"images": images, "cotangent": cotangent, "counts": counts, "master": master, "moment_one": moment_one, "moment_two": moment_two}


@jax.custom_vjp
def low(v):
    return lax.optimization_barrier(v.astype(jnp.bfloat16)).astype(jnp.float32)

@jax.custom_vjp
def low_back(v):
    return v

def low_keep(v):
    return (low(v), None)

def low_pass(kept, grad):
    return (grad,)

def back_keep(v):
    return (v, None)

def back_low(kept, grad):
    return (low(grad),)
low.defvjp(low_keep, low_pass)
low_back.defvjp(back_keep, back_low)
highest = lax.Precision.HIGHEST
beta_one = 0.9
beta_two = 0.999
learn_rate = 0.05
decay_rate = 0.05
epsilon = 1e-08

def param_shapes():
    return [(D,)] * 8 + [(FF,), (D, 3 * D), (D, D), (D, FF), (FF, D)]

def unpack(flat):
    pieces = []
    offset = 0
    for shape in param_shapes():
        count = math.prod(shape)
        pieces.append(flat[offset:offset + count].reshape(shape))
        offset += count
    return pieces

def layer_norm(values, gain, shift):
    centered = values - lax.optimization_barrier(jnp.mean(values, axis=-1, keepdims=True))
    spread = lax.optimization_barrier(jnp.mean(centered * centered, axis=-1, keepdims=True))
    return centered * lax.rsqrt(spread + 1e-06) * gain + shift

def layer_forward(params, inputs):
    gain_one, bias_one, query_bias, value_bias, out_bias, gain_two, bias_two, down_bias, up_bias, qkv_weight, out_weight, up_weight, down_weight = params
    batch, length = (inputs.shape[0], inputs.shape[1])
    normed = low(layer_norm(inputs, gain_one, bias_one))
    qkv_bias = jnp.concatenate([query_bias, jnp.zeros_like(query_bias), value_bias])
    projected = jnp.einsum('bsd,de->bse', normed, qkv_weight, precision=highest) + qkv_bias
    projected = low(low_back(projected))
    queries = projected[..., :D].reshape(batch, length, H, HD)
    keys = projected[..., D:2 * D].reshape(batch, length, H, HD)
    values = projected[..., 2 * D:].reshape(batch, length, H, HD)
    scores = low_back(jnp.einsum('bqhd,bkhd->bhqk', queries, keys, precision=highest) * HD ** (-0.5))
    probs = low(jax.nn.softmax(scores, axis=-1))
    attended = jnp.einsum('bhqk,bkhd->bqhd', probs, values, precision=highest).reshape(batch, length, D)
    attended = low(low_back(attended))
    branch = low_back(jnp.einsum('bsd,de->bse', attended, out_weight, precision=highest) + out_bias)
    middle = inputs + branch
    normed_two = low(layer_norm(middle, gain_two, bias_two))
    hidden = low_back(jnp.einsum('bsd,df->bsf', normed_two, up_weight, precision=highest) + up_bias)
    activated = low(jax.nn.gelu(hidden, approximate=False))
    mixed = low_back(jnp.einsum('bsf,fd->bsd', activated, down_weight, precision=highest) + down_bias)
    return middle + mixed

def run_layers(stacked, inputs):
    for level_index in range(LAYERS):
        inputs = layer_forward(unpack(stacked[level_index]), inputs)
    return inputs

def reference(images, cotangent, counts, master, moment_one, moment_two):
    weights_low = lax.optimization_barrier(master.astype(jnp.bfloat16)).astype(jnp.float32)
    slot_ids = jnp.arange(SLOTS * N_FSDP)
    live = ((slot_ids % SLOTS)[None, :] < counts[:, slot_ids // SLOTS]).astype(jnp.float32)
    per_group = 16
    groups = MICRO * SLOTS * N_FSDP // per_group
    inputs = images.astype(jnp.float32).reshape(groups, per_group, SEQ, D)
    seeds = cotangent.astype(jnp.float32).reshape(groups, per_group, SEQ, D)
    masks = live.reshape(groups, per_group)
    checked = jax.checkpoint(run_layers)

    def total(stacked, group_inputs):

        def visit(carry, block):
            group_in, group_seed, group_mask = block
            outs = checked(stacked, group_in)
            return (carry + jnp.sum(outs * group_seed * group_mask[:, None, None]), outs)
        loss_sum, outs = lax.scan(visit, jnp.zeros((), jnp.float32), (group_inputs, seeds, masks))
        return (loss_sum, outs)
    loss_sum, pullback, outs = jax.vjp(total, weights_low, inputs, has_aux=True)
    grad_flat, grad_inputs = pullback(jnp.ones_like(loss_sum))
    weight_grad = grad_flat / IMAGES
    activations = (outs.reshape(MICRO, SLOTS * N_FSDP, SEQ, D) * live[:, :, None, None]).astype(jnp.bfloat16)
    input_grad = grad_inputs.reshape(MICRO, SLOTS * N_FSDP, SEQ, D)
    first_new = beta_one * moment_one + (1.0 - beta_one) * weight_grad
    second_new = beta_two * moment_two + (1.0 - beta_two) * weight_grad * weight_grad
    update = first_new / (1.0 - beta_one ** STEP) / (jnp.sqrt(second_new / (1.0 - beta_two ** STEP)) + epsilon)
    new_master = master - learn_rate * (update + decay_rate * master)
    return (activations, input_grad, weight_grad, new_master, first_new, second_new)
```

```python
import functools
import math

import jax
import jax.numpy as jnp
from jax import lax
from jax.experimental import pallas as pl
from jax.experimental.pallas import tpu as pltpu
from jax.sharding import PartitionSpec as P

D = 384
H = 6
HD = 64
FF = 1536
SEQ = 197
STEP = 3
TP = 208
QP = 256

beta_one = 0.9
beta_two = 0.999
learn_rate = 0.05
decay_rate = 0.05
epsilon = 1e-08

f32 = jnp.float32
bf = jnp.bfloat16
R_QKV, R_P, R_U, R_D, R_END = 36, 3492, 4644, 9252, 13860
NN = (((1,), (0,)), ((), ()))
NT = (((1,), (1,)), ((), ()))
TN = (((0,), (0,)), ((), ()))
G1, B1, BQ, BV, BP, G2, B2, BD, BU = range(9)


def dot(a, b, dims):
    return lax.dot_general(a, b, dims, preferred_element_type=f32)


def wide(r):
    return jnp.concatenate([r, r, r], axis=1)


def rowsum(x):
    return jnp.sum(x, 0, keepdims=True)


def norm(x):
    m = jnp.sum(x, -1, keepdims=True) * (1.0 / D)
    c = x - m
    v = jnp.sum(c * c, -1, keepdims=True) * (1.0 / D)
    r = lax.rsqrt(v + 1e-6)
    return c * r, jnp.broadcast_to(r, (x.shape[0], 128))


def norm_back(dh, n, r, g, dy):
    e = dh * g
    me = jnp.sum(e, -1, keepdims=True) * (1.0 / D)
    men = jnp.sum(e * n, -1, keepdims=True) * (1.0 / D)
    return dy + (e - me - n * men) * wide(r)


def half_mask(rows, e):
    lane = lax.broadcasted_iota(jnp.int32, (rows, 128), 1)
    return (lane < 64) if e == 0 else (lane >= 64)


def keep(mask, v):
    return jnp.where(mask, v, jnp.zeros_like(v))


class NS:
    pass


SAVED = [
    ("N1", (TP, D), bf),
    ("R1", (TP, 128), f32),
    ("Q", (QP, D), bf),
    ("KV", (TP, 2 * D), bf),
    ("PT", (H, TP, QP), bf),
    ("O", (TP, D), bf),
    ("N2", (TP, D), bf),
    ("R2", (TP, 128), f32),
    ("GB", (TP, FF), bf),
    ("GP", (TP, FF), bf),
]


def unpack_layer(S, l, nd, rows):
    wg, F, V = S.wg.at[l], S.F, S.V.at[l]

    def put(d, c):
        F[pl.ds(rows * d, rows), :] = wg[d, 0:rows, :].astype(f32)
        return c

    lax.fori_loop(0, nd, put, 0)
    for k in range(8):
        for j in range(3):
            V[k : k + 1, 128 * j : 128 * j + 128] = F[3 * k + j : 3 * k + j + 1, :]
    for j in range(12):
        V[8:9, 128 * j : 128 * j + 128] = F[24 + j : 25 + j, :]
    for W, off, h, w in ((S.Wq, R_QKV, D, 3 * D), (S.Wp, R_P, D, D), (S.Wu, R_U, D, FF), (S.Wd, R_D, FF, D)):
        n = w // 128
        for j in range(n):
            W[l, :, 128 * j : 128 * j + 128] = F[pl.ds(off + j, h, stride=n), :].astype(bf)


def fwd_attention(S, l, i):
    V = S.V
    n1, r1 = norm(S.X[i])
    S.N1[l, i] = n1.astype(bf)
    S.R1[l, i] = r1
    h = (n1 * V[l, G1 : G1 + 1, 0:D] + V[l, B1 : B1 + 1, 0:D]).astype(bf)
    qkv = dot(h, S.Wq[l], NN)
    S.Q[l, i, 0:TP, :] = (qkv[:, 0:D] + V[l, BQ : BQ + 1, 0:D]).astype(bf)
    S.KV[l, i, :, 0:D] = qkv[:, D : 2 * D].astype(bf)
    S.KV[l, i, :, D : 2 * D] = (qkv[:, 2 * D :] + V[l, BV : BV + 1, 0:D]).astype(bf)
    row = lax.broadcasted_iota(jnp.int32, (TP, QP), 0)
    for p in range(3):
        kp = S.KV[l, i, :, 128 * p : 128 * p + 128] * jnp.asarray(0.125, bf)
        vp = S.KV[l, i, :, D + 128 * p : D + 128 * p + 128]
        qp = S.Q[l, i, :, 128 * p : 128 * p + 128]
        o = None
        for e in range(2):
            m = half_mask(TP, e)
            s = dot(keep(m, kp), qp, NT)
            s = jnp.where(row < SEQ, s, -1e30)
            ex = jnp.exp(s - jnp.max(s, 0, keepdims=True))
            pb = (ex * (1.0 / jnp.sum(ex, 0, keepdims=True))).astype(bf)
            S.PT[l, i, 2 * p + e] = pb
            oo = dot(pb, keep(m, vp), TN)
            o = oo if o is None else o + oo
        S.O[l, i, :, 128 * p : 128 * p + 128] = o[0:TP].astype(bf)


def fwd_mlp(S, l, i):
    V = S.V
    x1 = S.X[i] + dot(S.O[l, i], S.Wp[l], NN) + V[l, BP : BP + 1, 0:D]
    n2, r2 = norm(x1)
    S.N2[l, i] = n2.astype(bf)
    S.R2[l, i] = r2
    h2 = (n2 * V[l, G2 : G2 + 1, 0:D] + V[l, B2 : B2 + 1, 0:D]).astype(bf)
    for c in range(3):
        sl = slice(512 * c, 512 * c + 512)
        u = dot(h2, S.Wu[l, :, sl], NN) + V[l, BU : BU + 1, sl]
        phi = 0.5 + 0.5 * lax.erf(u * math.sqrt(0.5))
        S.GB[l, i, :, sl] = (u * phi).astype(bf)
        S.GP[l, i, :, sl] = (phi + u * (jnp.exp(u * u * -0.5) * (1.0 / math.sqrt(2 * math.pi)))).astype(bf)
    S.X[i] = x1 + dot(S.GB[l, i], S.Wd[l], NN) + V[l, BD : BD + 1, 0:D]


def bwd_mlp(S, l, i):
    V, VG = S.V, S.VG
    dy = S.DX[i]
    dm = dy.astype(bf)
    S.DM[i] = dm
    VG[BD : BD + 1, 0:D] += rowsum(dy)
    for c in range(3):
        sl = slice(512 * c, 512 * c + 512)
        du = dot(dm, S.Wd[l, sl, :], NT) * S.GP[l, i, :, sl].astype(f32)
        VG[BU : BU + 1, sl] += rowsum(du)
        S.GP[l, i, :, sl] = du.astype(bf)
    dh2 = dot(S.GP[l, i], S.Wu[l], NT)
    n2 = S.N2[l, i].astype(f32)
    VG[G2 : G2 + 1, 0:D] += rowsum(dh2 * n2)
    VG[B2 : B2 + 1, 0:D] += rowsum(dh2)
    dx1 = norm_back(dh2, n2, S.R2[l, i], V[l, G2 : G2 + 1, 0:D], dy)
    VG[BP : BP + 1, 0:D] += rowsum(dx1)
    S.DA[i] = dx1.astype(bf)
    S.DX[i] = dx1


def bwd_attention(S, l, i):
    V, VG = S.V, S.VG
    S.DO[0:TP, :] = dot(S.DA[i], S.Wp[l], NT).astype(bf)
    eighth = jnp.asarray(0.125, bf)
    for p in range(3):
        kp = S.KV[l, i, :, 128 * p : 128 * p + 128] * eighth
        vp = S.KV[l, i, :, D + 128 * p : D + 128 * p + 128]
        qp = S.Q[l, i, :, 128 * p : 128 * p + 128] * eighth
        do = S.DO[:, 128 * p : 128 * p + 128]
        dq = dk = dv = None
        for e in range(2):
            m = half_mask(TP, e)
            mq = half_mask(QP, e)
            pb = S.PT[l, i, 2 * p + e]
            dp = dot(keep(m, vp), do, NT)
            pf = pb.astype(f32)
            t = pf * dp
            ds = (t - pf * rowsum(t)).astype(bf)
            a = dot(pb, keep(mq, do), NN)
            b = dot(ds, keep(mq, qp), NN)
            c = dot(ds, keep(m, kp), TN)
            dv = a if dv is None else dv + a
            dk = b if dk is None else dk + b
            dq = c if dq is None else dq + c
        dq = dq[0:TP]
        sl = slice(128 * p, 128 * p + 128)
        VG[BQ : BQ + 1, sl] += rowsum(dq)
        VG[BV : BV + 1, sl] += rowsum(dv)
        S.DQKV[i, :, sl] = dq.astype(bf)
        S.DQKV[i, :, D + 128 * p : D + 128 * p + 128] = dk.astype(bf)
        S.DQKV[i, :, 2 * D + 128 * p : 2 * D + 128 * p + 128] = dv.astype(bf)
    dh = dot(S.DQKV[i], S.Wq[l], NT)
    n1 = S.N1[l, i].astype(f32)
    VG[G1 : G1 + 1, 0:D] += rowsum(dh * n1)
    VG[B1 : B1 + 1, 0:D] += rowsum(dh)
    S.DX[i] = norm_back(dh, n1, S.R1[l, i], V[l, G1 : G1 + 1, 0:D], S.DX[i])


def flat(v):
    return v.reshape(v.shape[0] * v.shape[1], v.shape[2])


def store_grad(F, val, first, n):
    for j in range(val.shape[1] // 128):
        F[pl.ds(first + j, val.shape[0], stride=n), :] = val[:, 128 * j : 128 * j + 128]


def grads_mlp(S, l):
    V, F = S.V, S.F
    dm = flat(S.DM[...])
    for c in range(3):
        gb = flat(S.GB[l, :, :, 512 * c : 512 * c + 512])
        store_grad(F, dot(gb, dm, TN), R_D + 3 * 512 * c, 3)
    h2 = (flat(S.N2[l]).astype(f32) * V[l, G2 : G2 + 1, 0:D] + V[l, B2 : B2 + 1, 0:D]).astype(bf)
    for c in range(3):
        du = flat(S.GP[l, :, :, 512 * c : 512 * c + 512])
        store_grad(F, dot(h2, du, TN), R_U + 4 * c, 12)


def grads_attention(S, l):
    V, VG, F = S.V, S.VG, S.F
    store_grad(F, dot(flat(S.O[l]), flat(S.DA[...]), TN), R_P, 3)
    h = (flat(S.N1[l]).astype(f32) * V[l, G1 : G1 + 1, 0:D] + V[l, B1 : B1 + 1, 0:D]).astype(bf)
    for c0, c1 in ((0, 512), (512, 1024), (1024, 1152)):
        store_grad(F, dot(h, flat(S.DQKV[:, :, c0:c1]), TN), R_QKV + c0 // 128, 9)
    for k in range(8):
        for j in range(3):
            F[3 * k + j : 3 * k + j + 1, :] = VG[k : k + 1, 128 * j : 128 * j + 128]
    for j in range(12):
        F[24 + j : 25 + j, :] = VG[8:9, 128 * j : 128 * j + 128]


def topology(mesh):
    devices = list(mesh.devices.flat)
    where = {}
    for index, device in enumerate(devices):
        where[tuple(device.coords) + (device.core_on_chip,)] = index
    sizes = [max(key[a] for key in where) - min(key[a] for key in where) + 1 for a in range(4)]
    origin = [min(key[a] for key in where) for a in range(4)]
    dims = []
    for a in range(4):
        if sizes[a] > 1:
            step = list(origin)
            step[a] += 1
            dims.append((int(sizes[a]), int(where[tuple(step)] - where[tuple(origin)])))
        else:
            dims.append((1, 1))
    for key, index in where.items():
        assert index == sum((key[a] - origin[a]) * dims[a][1] for a in range(4))
    chip = sorted(dims[:3], key=lambda d: -d[0])
    return tuple(chip) + (dims[3],)


class Net:
    def __init__(self, topo):
        self.topo = topo
        self.me = lax.axis_index("fsdp")
        self.at = [lax.rem(lax.div(self.me, stride), size) for size, stride in topo]

    def move(self, index, axis, by):
        size, stride = self.topo[axis]
        if by == 0 or size == 1:
            return index
        return index + (lax.rem(self.at[axis] + by, size) - self.at[axis]) * stride

    def block(self, offsets):
        index = self.me
        for axis, by in offsets.items():
            index = self.move(index, axis, by)
        return index

    def peers(self):
        out = []
        for axis, (size, _) in enumerate(self.topo):
            out += [self.move(self.me, axis, by) for by in range(1, size)]
        return out


def remote(src, dst, send, recv, peer):
    return pltpu.make_async_remote_copy(
        src_ref=src, dst_ref=dst, send_sem=send, recv_sem=recv, device_id=(peer,), device_id_type=pl.DeviceIdType.MESH
    )


def halves(RP):
    first = 16 * ((RP // 16 + 1) // 2)
    return ((0, first), (first, RP - first))


def gather_events(net, wg, send, recv):
    RP = wg.shape[1]
    cut = halves(RP)
    nz, n1, n2, nc = [size for size, _ in net.topo]
    orders = ((1, 2), (2, 1))

    def copy(c, blk, peer):
        first, count = cut[c]
        ref = wg.at[blk, pl.ds(first, count), :]
        return remote(ref, ref, send, recv.at[c, blk], peer)

    def targets(axes):
        return [net.move(net.me, axis, by) for axis in axes for by in range(1, net.topo[axis][0])]

    def forward(c, blk, axes):
        for peer in targets(axes):
            copy(c, blk, peer).start()

    def arrived(c, blk, axes):
        ends = targets(axes)

        def run():
            copy(c, blk, net.me).wait_recv()
            for peer in ends:
                copy(c, blk, peer).start()

        return run

    events = []

    def start():
        for c in range(2):
            forward(c, net.me, (0,))
        for c in range(2):
            forward(c, net.me, orders[c])
        for c in range(2):
            forward(c, net.me, (3,))

    events.append((-1.0, start))
    for c in range(2):
        P, Q = orders[c]
        sp, sq = net.topo[P][0], net.topo[Q][0]
        for k in range(nz):
            if k:
                events.append((k, arrived(c, net.block({0: k}), (P, Q, 3))))
            for jp in range(1, sp):
                events.append((k + 1.1, arrived(c, net.block({0: k, P: jp}), (Q, 3))))
            for jq in range(1, sq):
                events.append((k + 1.2, arrived(c, net.block({0: k, Q: jq}), (3,))))
                for jp in range(1, sp):
                    events.append((k + 2.3, arrived(c, net.block({0: k, P: jp, Q: jq}), (3,))))
        for k in range(nz):
            for a in range(n1):
                for b in range(n2):
                    for w in range(1, nc):
                        blk = net.block({0: k, 1: a, 2: b, 3: w})
                        events.append((99.0, arrived(c, blk, ())))
    events.sort(key=lambda e: e[0])
    return [e[1] for e in events]


def wait_sends(buf, send, blocks):
    ref = buf.at[pl.ds(0, blocks)]
    pltpu.make_async_copy(ref, ref, send).wait()


def scatter_events(net, G, RB, send, recv):
    RP = G.shape[1]
    cut = halves(RP)
    nz, n1, n2, nc = [size for size, _ in net.topo]
    orders = ((2, 1), (1, 2))
    pending = []

    def flush():
        for start in pending:
            start()
        del pending[:]

    def rows(c):
        return pl.ds(cut[c][0], cut[c][1])

    def add(ref, blk, c):
        G[blk, rows(c), :] = G[blk, rows(c), :] + ref[...]

    def place(off, axis):
        return lax.rem(net.at[axis] + off[axis], net.topo[axis][0])

    def core_sum(off):
        blk = net.block(off)
        s = (place(off, 0) * n1 + place(off, 1)) * n2 + place(off, 2)
        sends = []
        for c in range(2):
            Q, P = orders[c]
            by = off[Q]
            if by:
                spot = place(off, 0) * net.topo[P][0] + place(off, P)
                peer = net.move(net.me, Q, by)
                sends.append((c, by - 1, spot, peer))

        def run():
            for w in range(1, nc):
                remote(RB[0].at[w - 1, s], RB[0].at[w - 1, s], send, recv[0].at[w - 1, s], net.me).wait_recv()
            for c in range(2):
                for w in range(1, nc):
                    add(RB[0].at[w - 1, s, rows(c), :], blk, c)
            flush()
            for c, by, spot, peer in sends:
                pending.append(lambda c=c, by=by, spot=spot, peer=peer: remote(
                    G.at[blk, rows(c), :], RB[1][c].at[by, spot], send, recv[1][c].at[by, spot], peer).start())

        return run

    def second(c, off):
        Q, P = orders[c]
        blk = net.block(off)
        at_z = place(off, 0)
        spot = at_z * net.topo[P][0] + place(off, P)
        by = off[P]
        peer = net.move(net.me, P, by)

        def run():
            for j in range(net.topo[Q][0] - 1):
                ref = RB[1][c].at[j, spot]
                remote(ref, ref, send, recv[1][c].at[j, spot], net.me).wait_recv()
                add(ref, blk, c)
            flush()
            if by:
                pending.append(lambda: remote(
                    G.at[blk, rows(c), :], RB[2][c].at[by - 1, at_z], send, recv[2][c].at[by - 1, at_z], peer).start())

        return run

    def third(c, off):
        Q, P = orders[c]
        blk = net.block(off)
        at_z = place(off, 0)
        by = off[0]
        peer = net.move(net.me, 0, by)

        def run():
            for j in range(net.topo[P][0] - 1):
                ref = RB[2][c].at[j, at_z]
                remote(ref, ref, send, recv[2][c].at[j, at_z], net.me).wait_recv()
                add(ref, blk, c)
            flush()
            if by:
                pending.append(lambda: remote(
                    G.at[blk, rows(c), :], RB[3][c].at[by - 1], send, recv[3][c].at[by - 1], peer).start())

        return run

    def last():
        flush()
        for c in range(2):
            for by in range(1, nz):
                ref = RB[3][c].at[by - 1]
                remote(ref, ref, send, recv[3][c].at[by - 1], net.me).wait_recv()

    events = []
    z_order = [k for k in range(1, nz)] + [0]
    plane = sorted(((a, b) for a in range(n1) for b in range(n2)), key=lambda ab: -((ab[0] > 0) + (ab[1] > 0)))
    for r, k in enumerate(z_order):
        for a, b in plane:
            events.append((r, core_sum({0: k, 1: a, 2: b})))
        for c in range(2):
            Q, P = orders[c]
            for j in list(range(1, net.topo[P][0])) + [0]:
                events.append((r + 1.5 + 0.1 * (j == 0), second(c, {0: k, P: j, Q: 0})))
            events.append((r + 2.7, third(c, {0: k, P: 0, Q: 0})))
    events.sort(key=lambda e: e[0])
    return [e[1] for e in events] + [last], flush


def pack_and_send(net, S, G, RB, send, recv, nd, rows):
    nz, n1, n2, nc = [size for size, _ in net.topo]
    F = S.F

    def chip(t):
        a = lax.div(t, n1 * n2)
        b = lax.rem(lax.div(t, n2), n1)
        g = lax.rem(t, n2)
        base = a * net.topo[0][1] + b * net.topo[1][1] + g * net.topo[2][1]
        return base

    def pack(blk):
        G[blk, 0:rows, :] = F[pl.ds(rows * blk, rows), :].astype(bf)

    def go(t, w):
        blk = chip(t) + lax.rem(net.at[3] + w, nc) * net.topo[3][1]
        remote(G.at[blk], RB[0].at[w - 1, t], send, recv[0].at[w - 1, t], net.move(net.me, 3, w)).start()

    total = nz * n1 * n2
    for w in range(1, nc):
        def step(t, c):
            pack(chip(t) + lax.rem(net.at[3] + w, nc) * net.topo[3][1])

            @pl.when(t > 0)
            def _():
                go(t - 1, w)

            return c

        lax.fori_loop(0, total, step, 0)

    def mine(t, c):
        pack(chip(t) + net.at[3] * net.topo[3][1])
        return c

    lax.fori_loop(0, total, mine, 0)
    for w in range(1, nc):
        go(total - 1, w)


def spread(events, points):
    n = len(events)
    return [events[n * p // points : n * (p + 1) // points] for p in range(points)]


def at_points(groups, index, flush):
    for value, group in enumerate(groups):
        if group:

            @pl.when(index == value)
            def _(group=group):
                for event in group:
                    event()
                flush()


def kernel(cfg, counts, images, cotangent, master, one, two, act, dimg, o_grad, o_master, o_one, o_two, *scr):
    topo, L, NI, nd, rows, slots = cfg
    S = NS()
    for name, ref in zip(NAMES, scr):
        setattr(S, name, ref)
    S.wg = S.wgs
    net = Net(topo)

    barrier = pltpu.get_barrier_semaphore()
    peers = net.peers()
    for peer in peers:
        pl.semaphore_signal(barrier, inc=1, device_id=(peer,), device_id_type=pl.DeviceIdType.MESH)

    loads = [
        pltpu.make_async_copy(master, S.vm, S.lsem.at[0]),
        pltpu.make_async_copy(images, S.vimg, S.lsem.at[1]),
        pltpu.make_async_copy(cotangent, S.vcot, S.lsem.at[2]),
        pltpu.make_async_copy(one, S.v1, S.lsem.at[3]),
        pltpu.make_async_copy(two, S.v2, S.lsem.at[4]),
    ]
    for load in loads:
        load.start()
    loads[0].wait()
    for l in range(L):
        S.wg[l, net.me, 0:rows, :] = S.vm[:, l, :].astype(bf)
    pl.semaphore_wait(barrier, len(peers))

    gathers = [gather_events(net, S.wg.at[l], S.gsend.at[l], S.grecv.at[l]) for l in range(L)]
    split = len(gathers[0])
    gathers[0][0]()

    def live(i):
        return lax.rem(i, slots) < counts[lax.div(i, slots), 0]

    loads[1].wait()
    loads[2].wait()
    edge = SEQ - SEQ % 16

    def init(i, c):
        S.X[i, edge:, :] = jnp.zeros((TP - edge, D), f32)
        S.DX[i, edge:, :] = jnp.zeros((TP - edge, D), f32)
        S.X[i, 0:SEQ, :] = S.vimg[i].astype(f32)
        S.DX[i, 0:SEQ, :] = jnp.where(live(i), S.vcot[i].astype(f32), 0.0)
        for l in range(L):
            S.Q[l, i, TP:, :] = jnp.zeros((QP - TP, D), bf)
        return c

    lax.fori_loop(0, NI, init, 0)
    S.DO[TP:, :] = jnp.zeros((QP - TP, D), bf)

    for event in gathers[0][1:]:
        event()
    unpack_layer(S, 0, nd, rows)

    def nothing():
        pass

    flush = nothing
    for l in range(L):
        groups = []
        if l + 1 < L:
            gathers[l + 1][0]()
            groups = spread(gathers[l + 1][1:], 2 * NI)

        def forward(i, c):
            fwd_attention(S, l, i)
            at_points(groups[0::2], i, flush)
            fwd_mlp(S, l, i)
            at_points(groups[1::2], i, flush)
            return c

        lax.fori_loop(0, NI, forward, 0)
        if l + 1 < L:
            unpack_layer(S, l + 1, nd, rows)

    def finish(i, c):
        S.vimg[i] = jnp.where(live(i), S.X[i, 0:SEQ, :], 0.0).astype(bf)
        return c

    lax.fori_loop(0, NI, finish, 0)
    out_act = pltpu.make_async_copy(S.vimg, act, S.lsem.at[1])
    out_act.start()
    for l in range(L):
        wait_sends(S.wg.at[l], S.gsend.at[l], nd - 1)

    S.F[R_END:, :] = jnp.zeros((nd * rows - R_END, 128), f32)
    RB = [S.rb0, [S.rb1a, S.rb1b], [S.rb2a, S.rb2b], [S.rb3a, S.rb3b]]

    def recv_of(l):
        return [S.rr0.at[l], [S.rr1.at[l, c] for c in range(2)], [S.rr2.at[l, c] for c in range(2)], [S.rr3.at[l, c] for c in range(2)]]

    def adam(l):
        wait_sends(S.wg.at[l], S.rsend.at[l], nd - 1)
        g = []
        for c, (first, count) in enumerate(halves(S.wg.shape[2])):
            part = S.wg[l, net.me, pl.ds(first, count), :].astype(f32)
            for by in range(topo[0][0] - 1):
                part = part + RB[3][c][by].astype(f32)
            g.append(part)
        g = jnp.concatenate(g, axis=0)[0:rows] * (1.0 / (NI * nd))
        m1 = beta_one * S.v1[:, l, :] + (1.0 - beta_one) * g
        m2 = beta_two * S.v2[:, l, :] + (1.0 - beta_two) * g * g
        w = S.vm[:, l, :]
        update = m1 / (1.0 - beta_one**STEP) / (jnp.sqrt(m2 / (1.0 - beta_two**STEP)) + epsilon)
        S.vg[:, l, :] = g
        S.v1[:, l, :] = m1
        S.v2[:, l, :] = m2
        S.vm[:, l, :] = w - learn_rate * (update + decay_rate * w)

    loads[3].wait()
    loads[4].wait()
    pend, flush = [], nothing
    for l in reversed(range(L)):
        groups = spread(pend, 2 * NI)
        S.VG[...] = jnp.zeros_like(S.VG)

        def backward(i, c):
            bwd_mlp(S, l, i)
            at_points(groups[0::2], i, flush)
            bwd_attention(S, l, i)
            at_points(groups[1::2], i, flush)
            return c

        lax.fori_loop(0, NI, backward, 0)
        if l + 1 < L:
            adam(l + 1)
            for peer in peers:
                pl.semaphore_signal(S.credit, inc=1, device_id=(peer,), device_id_type=pl.DeviceIdType.MESH)
        grads_mlp(S, l)
        grads_attention(S, l)
        if l + 1 < L:
            pl.semaphore_wait(S.credit, len(peers))
        recv = recv_of(l)
        pack_and_send(net, S, S.wg.at[l], RB, S.rsend.at[l], recv, nd, rows)
        pend, flush = scatter_events(net, S.wg.at[l], RB, S.rsend.at[l], recv)

    def fin(i, c):
        S.vdx[i] = S.DX[i, 0:SEQ, :]
        return c

    lax.fori_loop(0, NI, fin, 0)
    out_dx = pltpu.make_async_copy(S.vdx, dimg, S.lsem.at[2])
    out_dx.start()
    for event in pend:
        event()
    adam(0)
    outs = [
        pltpu.make_async_copy(S.vm, o_master, S.lsem.at[0]),
        pltpu.make_async_copy(S.vg, o_grad, S.lsem.at[5]),
        pltpu.make_async_copy(S.v1, o_one, S.lsem.at[3]),
        pltpu.make_async_copy(S.v2, o_two, S.lsem.at[4]),
    ]
    for out in outs:
        out.start()
    out_act.wait()
    out_dx.wait()
    for out in outs:
        out.wait()


NAMES = (
    ["Wq", "Wp", "Wu", "Wd", "V", "VG", "F", "X", "DX", "DO", "DM", "DA", "DQKV", "wgs"]
    + [name for name, _, _ in SAVED]
    + ["rb0", "rb1a", "rb1b", "rb2a", "rb2b", "rb3a", "rb3b"]
    + ["vm", "v1", "v2", "vg", "vimg", "vcot", "vdx"]
    + ["lsem", "gsend", "grecv", "rsend", "rr0", "rr1", "rr2", "rr3", "credit"]
)


def body(topo, images, cotangent, counts, master, moment_one, moment_two):
    micro, slots = images.shape[:2]
    NI = micro * slots
    L, width = master.shape
    rows = width // 128
    RP = 16 * ((rows + 15) // 16)
    nd = lax.axis_size("fsdp")
    (nz, _), (n1, _), (n2, _), (nc, _) = topo
    cut = halves(RP)

    def rows_of(v):
        return v.reshape(L, rows, 128).transpose(1, 0, 2)

    def back(v):
        return v.transpose(1, 0, 2).reshape(L, width)

    VM, DMA = pltpu.VMEM, pltpu.SemaphoreType.DMA
    scratch = [
        VM((L, D, 3 * D), bf),
        VM((L, D, D), bf),
        VM((L, D, FF), bf),
        VM((L, FF, D), bf),
        VM((L, 16, FF), f32),
        VM((16, FF), f32),
        VM((nd * rows, 128), f32),
        VM((NI, TP, D), f32),
        VM((NI, TP, D), f32),
        VM((QP, D), bf),
        VM((NI, TP, D), bf),
        VM((NI, TP, D), bf),
        VM((NI, TP, 3 * D), bf),
        VM((L, nd, RP, 128), bf),
    ]
    scratch += [VM((L, NI) + shape, kind) for _, shape, kind in SAVED]
    scratch += [VM((max(nc - 1, 1), nz * n1 * n2, RP, 128), bf)]
    scratch += [
        VM((n2 - 1, nz * n1, cut[0][1], 128), bf),
        VM((n1 - 1, nz * n2, cut[1][1], 128), bf),
        VM((n1 - 1, nz, cut[0][1], 128), bf),
        VM((n2 - 1, nz, cut[1][1], 128), bf),
        VM((nz - 1, cut[0][1], 128), bf),
        VM((nz - 1, cut[1][1], 128), bf),
    ]
    scratch += [VM((rows, L, 128), f32)] * 4
    scratch += [VM((NI, SEQ, D), bf), VM((NI, SEQ, D), bf), VM((NI, SEQ, D), f32)]
    wide_first = max(n1, n2) - 1
    scratch += [
        DMA((6,)),
        DMA((L,)),
        DMA((L, 2, nd)),
        DMA((L,)),
        DMA((L, max(nc - 1, 1), nz * n1 * n2)),
        DMA((L, 2, wide_first, nz * max(n1, n2))),
        DMA((L, 2, wide_first, nz)),
        DMA((L, 2, nz - 1)),
        pltpu.SemaphoreType.REGULAR,
    ]
    anywhere = pl.BlockSpec(memory_space=pl.ANY)
    state = jax.ShapeDtypeStruct((rows, L, 128), f32)
    shape = (NI, SEQ, D)
    out = pl.pallas_call(
        functools.partial(kernel, (topo, L, NI, nd, rows, slots)),
        out_shape=(jax.ShapeDtypeStruct(shape, bf), jax.ShapeDtypeStruct(shape, f32), state, state, state, state),
        in_specs=[pl.BlockSpec(memory_space=pltpu.SMEM)] + [anywhere] * 5,
        out_specs=(anywhere,) * 6,
        scratch_shapes=scratch,
        compiler_params=pltpu.CompilerParams(vmem_limit_bytes=67043328, collective_id=0, has_side_effects=True),
        name="step",
    )(
        counts,
        images.reshape(shape),
        cotangent.reshape(shape),
        rows_of(master),
        rows_of(moment_one),
        rows_of(moment_two),
    )
    return (
        out[0].reshape(images.shape),
        out[1].reshape(images.shape),
        back(out[2]),
        back(out[3]),
        back(out[4]),
        back(out[5]),
    )


def solution(mesh):
    topo = topology(mesh)
    tokens = P(None, "fsdp", None, None)
    state = P(None, "fsdp")
    return jax.shard_map(
        functools.partial(body, topo),
        mesh=mesh,
        in_specs=(tokens, tokens, state, state, state, state),
        out_specs=(tokens, tokens, state, state, state, state),
        check_vma=False,
    )
```

```python
import functools
import math

import jax
import jax.numpy as jnp
from jax import lax
from jax.experimental import pallas as pl
from jax.experimental.pallas import tpu as pltpu
from jax.sharding import PartitionSpec as P

D = 384
H = 6
HD = 64
FF = 1536
SEQ = 197
STEP = 3
TP = 208
QP = 256

beta_one = 0.9
beta_two = 0.999
learn_rate = 0.05
decay_rate = 0.05
epsilon = 1e-08

f32 = jnp.float32
bf = jnp.bfloat16
R_QKV, R_P, R_U, R_D, R_END = 36, 3492, 4644, 9252, 13860
NN = (((1,), (0,)), ((), ()))
NT = (((1,), (1,)), ((), ()))
TN = (((0,), (0,)), ((), ()))
G1, B1, BQ, BV, BP, G2, B2, BD, BU = range(9)


def dot(a, b, dims):
    return lax.dot_general(a, b, dims, preferred_element_type=f32)


def wide(r):
    return jnp.concatenate([r, r, r], axis=1)


def rowsum(x):
    return jnp.sum(x, 0, keepdims=True)


def norm(x):
    m = jnp.sum(x, -1, keepdims=True) * (1.0 / D)
    c = x - m
    v = jnp.sum(c * c, -1, keepdims=True) * (1.0 / D)
    r = lax.rsqrt(v + 1e-6)
    return c * r, jnp.broadcast_to(r, (x.shape[0], 128))


def norm_back(dh, n, r, g, dy):
    e = dh * g
    me = jnp.sum(e, -1, keepdims=True) * (1.0 / D)
    men = jnp.sum(e * n, -1, keepdims=True) * (1.0 / D)
    return dy + (e - me - n * men) * wide(r)


def half_mask(rows, e):
    lane = lax.broadcasted_iota(jnp.int32, (rows, 128), 1)
    return (lane < 64) if e == 0 else (lane >= 64)


def keep(mask, v):
    return jnp.where(mask, v, jnp.zeros_like(v))


class NS:
    pass


SAVED = [
    ("N1", (TP, D), bf),
    ("R1", (TP, 128), f32),
    ("Q", (QP, D), bf),
    ("KV", (TP, 2 * D), bf),
    ("PT", (H, TP, QP), bf),
    ("O", (TP, D), bf),
    ("N2", (TP, D), bf),
    ("R2", (TP, 128), f32),
    ("GB", (TP, FF), bf),
    ("GP", (TP, FF), bf),
]


def unpack_layer(S, l, nd, rows):
    wg, F, V = S.wg.at[l], S.F, S.V.at[l]

    def put(d, c):
        F[pl.ds(rows * d, rows), :] = wg[d, 0:rows, :].astype(f32)
        return c

    lax.fori_loop(0, nd, put, 0)
    for k in range(8):
        for j in range(3):
            V[k : k + 1, 128 * j : 128 * j + 128] = F[3 * k + j : 3 * k + j + 1, :]
    for j in range(12):
        V[8:9, 128 * j : 128 * j + 128] = F[24 + j : 25 + j, :]
    for W, off, h, w in ((S.Wq, R_QKV, D, 3 * D), (S.Wp, R_P, D, D), (S.Wu, R_U, D, FF), (S.Wd, R_D, FF, D)):
        n = w // 128
        for j in range(n):
            W[l, :, 128 * j : 128 * j + 128] = F[pl.ds(off + j, h, stride=n), :].astype(bf)


def fwd_attention(S, l, i):
    V = S.V
    n1, r1 = norm(S.X[i])
    S.N1[l, i] = n1.astype(bf)
    S.R1[l, i] = r1
    h = (n1 * V[l, G1 : G1 + 1, 0:D] + V[l, B1 : B1 + 1, 0:D]).astype(bf)
    qkv = dot(h, S.Wq[l], NN)
    S.Q[l, i, 0:TP, :] = (qkv[:, 0:D] + V[l, BQ : BQ + 1, 0:D]).astype(bf)
    S.KV[l, i, :, 0:D] = qkv[:, D : 2 * D].astype(bf)
    S.KV[l, i, :, D : 2 * D] = (qkv[:, 2 * D :] + V[l, BV : BV + 1, 0:D]).astype(bf)
    row = lax.broadcasted_iota(jnp.int32, (TP, QP), 0)
    for p in range(3):
        kp = S.KV[l, i, :, 128 * p : 128 * p + 128] * jnp.asarray(0.125, bf)
        vp = S.KV[l, i, :, D + 128 * p : D + 128 * p + 128]
        qp = S.Q[l, i, :, 128 * p : 128 * p + 128]
        o = None
        for e in range(2):
            m = half_mask(TP, e)
            s = dot(keep(m, kp), qp, NT)
            s = jnp.where(row < SEQ, s, -1e30)
            ex = jnp.exp(s - jnp.max(s, 0, keepdims=True))
            pb = (ex * (1.0 / jnp.sum(ex, 0, keepdims=True))).astype(bf)
            S.PT[l, i, 2 * p + e] = pb
            oo = dot(pb, keep(m, vp), TN)
            o = oo if o is None else o + oo
        S.O[l, i, :, 128 * p : 128 * p + 128] = o[0:TP].astype(bf)


def fwd_mlp(S, l, i):
    V = S.V
    x1 = S.X[i] + dot(S.O[l, i], S.Wp[l], NN) + V[l, BP : BP + 1, 0:D]
    n2, r2 = norm(x1)
    S.N2[l, i] = n2.astype(bf)
    S.R2[l, i] = r2
    h2 = (n2 * V[l, G2 : G2 + 1, 0:D] + V[l, B2 : B2 + 1, 0:D]).astype(bf)
    for c in range(3):
        sl = slice(512 * c, 512 * c + 512)
        u = dot(h2, S.Wu[l, :, sl], NN) + V[l, BU : BU + 1, sl]
        phi = 0.5 + 0.5 * lax.erf(u * math.sqrt(0.5))
        S.GB[l, i, :, sl] = (u * phi).astype(bf)
        S.GP[l, i, :, sl] = (phi + u * (jnp.exp(u * u * -0.5) * (1.0 / math.sqrt(2 * math.pi)))).astype(bf)
    S.X[i] = x1 + dot(S.GB[l, i], S.Wd[l], NN) + V[l, BD : BD + 1, 0:D]


def bwd_mlp(S, l, i):
    V, VG = S.V, S.VG
    dy = S.DX[i]
    dm = dy.astype(bf)
    S.DM[i] = dm
    VG[BD : BD + 1, 0:D] += rowsum(dy)
    for c in range(3):
        sl = slice(512 * c, 512 * c + 512)
        du = dot(dm, S.Wd[l, sl, :], NT) * S.GP[l, i, :, sl].astype(f32)
        VG[BU : BU + 1, sl] += rowsum(du)
        S.GP[l, i, :, sl] = du.astype(bf)
    dh2 = dot(S.GP[l, i], S.Wu[l], NT)
    n2 = S.N2[l, i].astype(f32)
    VG[G2 : G2 + 1, 0:D] += rowsum(dh2 * n2)
    VG[B2 : B2 + 1, 0:D] += rowsum(dh2)
    dx1 = norm_back(dh2, n2, S.R2[l, i], V[l, G2 : G2 + 1, 0:D], dy)
    VG[BP : BP + 1, 0:D] += rowsum(dx1)
    S.DA[i] = dx1.astype(bf)
    S.DX[i] = dx1


def bwd_attention(S, l, i):
    V, VG = S.V, S.VG
    S.DO[0:TP, :] = dot(S.DA[i], S.Wp[l], NT).astype(bf)
    eighth = jnp.asarray(0.125, bf)
    for p in range(3):
        kp = S.KV[l, i, :, 128 * p : 128 * p + 128] * eighth
        vp = S.KV[l, i, :, D + 128 * p : D + 128 * p + 128]
        qp = S.Q[l, i, :, 128 * p : 128 * p + 128] * eighth
        do = S.DO[:, 128 * p : 128 * p + 128]
        dq = dk = dv = None
        for e in range(2):
            m = half_mask(TP, e)
            mq = half_mask(QP, e)
            pb = S.PT[l, i, 2 * p + e]
            dp = dot(keep(m, vp), do, NT)
            pf = pb.astype(f32)
            t = pf * dp
            ds = (t - pf * rowsum(t)).astype(bf)
            a = dot(pb, keep(mq, do), NN)
            b = dot(ds, keep(mq, qp), NN)
            c = dot(ds, keep(m, kp), TN)
            dv = a if dv is None else dv + a
            dk = b if dk is None else dk + b
            dq = c if dq is None else dq + c
        dq = dq[0:TP]
        sl = slice(128 * p, 128 * p + 128)
        VG[BQ : BQ + 1, sl] += rowsum(dq)
        VG[BV : BV + 1, sl] += rowsum(dv)
        S.DQKV[i, :, sl] = dq.astype(bf)
        S.DQKV[i, :, D + 128 * p : D + 128 * p + 128] = dk.astype(bf)
        S.DQKV[i, :, 2 * D + 128 * p : 2 * D + 128 * p + 128] = dv.astype(bf)
    dh = dot(S.DQKV[i], S.Wq[l], NT)
    n1 = S.N1[l, i].astype(f32)
    VG[G1 : G1 + 1, 0:D] += rowsum(dh * n1)
    VG[B1 : B1 + 1, 0:D] += rowsum(dh)
    S.DX[i] = norm_back(dh, n1, S.R1[l, i], V[l, G1 : G1 + 1, 0:D], S.DX[i])


def flat(v):
    return v.reshape(v.shape[0] * v.shape[1], v.shape[2])


def store_grad(F, val, first, n):
    for j in range(val.shape[1] // 128):
        F[pl.ds(first + j, val.shape[0], stride=n), :] = val[:, 128 * j : 128 * j + 128]


def grads_mlp(S, l):
    V, F = S.V, S.F
    dm = flat(S.DM[...])
    for c in range(3):
        gb = flat(S.GB[l, :, :, 512 * c : 512 * c + 512])
        store_grad(F, dot(gb, dm, TN), R_D + 3 * 512 * c, 3)
    h2 = (flat(S.N2[l]).astype(f32) * V[l, G2 : G2 + 1, 0:D] + V[l, B2 : B2 + 1, 0:D]).astype(bf)
    for c in range(3):
        du = flat(S.GP[l, :, :, 512 * c : 512 * c + 512])
        store_grad(F, dot(h2, du, TN), R_U + 4 * c, 12)


def grads_attention(S, l):
    V, VG, F = S.V, S.VG, S.F
    store_grad(F, dot(flat(S.O[l]), flat(S.DA[...]), TN), R_P, 3)
    h = (flat(S.N1[l]).astype(f32) * V[l, G1 : G1 + 1, 0:D] + V[l, B1 : B1 + 1, 0:D]).astype(bf)
    for c0, c1 in ((0, 512), (512, 1024), (1024, 1152)):
        store_grad(F, dot(h, flat(S.DQKV[:, :, c0:c1]), TN), R_QKV + c0 // 128, 9)
    for k in range(8):
        for j in range(3):
            F[3 * k + j : 3 * k + j + 1, :] = VG[k : k + 1, 128 * j : 128 * j + 128]
    for j in range(12):
        F[24 + j : 25 + j, :] = VG[8:9, 128 * j : 128 * j + 128]


def topology(mesh):
    devices = list(mesh.devices.flat)
    where = {}
    for index, device in enumerate(devices):
        where[tuple(device.coords) + (device.core_on_chip,)] = index
    sizes = [max(key[a] for key in where) - min(key[a] for key in where) + 1 for a in range(4)]
    origin = [min(key[a] for key in where) for a in range(4)]
    dims = []
    for a in range(4):
        if sizes[a] > 1:
            step = list(origin)
            step[a] += 1
            dims.append((int(sizes[a]), int(where[tuple(step)] - where[tuple(origin)])))
        else:
            dims.append((1, 1))
    for key, index in where.items():
        assert index == sum((key[a] - origin[a]) * dims[a][1] for a in range(4))
    chip = sorted(dims[:3], key=lambda d: -d[0])
    return tuple(chip) + (dims[3],)


class Net:
    def __init__(self, topo):
        self.topo = topo
        self.me = lax.axis_index("fsdp")
        self.at = [lax.rem(lax.div(self.me, stride), size) for size, stride in topo]

    def move(self, index, axis, by):
        if by == 0 or self.topo[axis][0] == 1:
            return index
        return index + (self.partner(axis, by) - self.at[axis]) * self.topo[axis][1]

    def partner(self, axis, by):
        at, out, weight, size = self.at[axis], 0, 1, self.topo[axis][0]
        assert size & (size - 1) == 0
        while weight < size:
            bit = lax.rem(lax.div(at, weight), 2)
            out = out + weight * (1 - bit if by & weight else bit)
            weight *= 2
        return out

    def block(self, offsets):
        index = self.me
        for axis, by in offsets.items():
            index = self.move(index, axis, by)
        return index

    def peers(self):
        out = []
        for axis, (size, _) in enumerate(self.topo):
            out += [self.move(self.me, axis, by) for by in range(1, size)]
        return out


def remote(src, dst, send, recv, peer):
    return pltpu.make_async_remote_copy(
        src_ref=src, dst_ref=dst, send_sem=send, recv_sem=recv, device_id=(peer,), device_id_type=pl.DeviceIdType.MESH
    )


def halves(RP):
    first = 16 * ((RP // 16 + 1) // 2)
    return ((0, first), (first, RP - first))


def gather_plan(net, wg, send, recv):
    RP = wg.shape[1]
    cut = halves(RP)
    nz, n1, n2, nc = [size for size, _ in net.topo]
    orders = ((1, 2), (2, 1))
    plan = NS()

    def copy(c, blk, peer):
        first, count = cut[c]
        ref = wg.at[blk, pl.ds(first, count), :]
        return remote(ref, ref, send, recv.at[c, blk], peer)

    def wait(c, blk):
        return lambda: copy(c, blk, net.me).wait_recv()

    def give(c, blk, axis):
        ends = [net.move(net.me, axis, by) for by in range(1, net.topo[axis][0])]

        def run():
            for peer in ends:
                copy(c, blk, peer).start()

        return run

    def every(*steps):
        def run():
            for step in steps:
                step()

        return run

    plan.along = every(*[every(*[
        (lambda c=c, peer=peer: copy(c, net.me, peer).start()) for c in range(2)]) for peer in [net.move(net.me, 0, by) for by in range(1, nz)]])
    plan.land, plan.near, plan.far, plan.core = [], [], [], []
    plan.second, plan.third, plan.corner = [], [], []
    for k in range(nz):
        blk = net.block({0: k})
        plan.land.append(every(*[wait(c, blk) for c in range(2)]) if k else every())
        plan.near.append(every(*[give(c, blk, orders[c][0]) for c in range(2)]))
        plan.far.append(every(*[give(c, blk, orders[c][1]) for c in range(2)]))
        plan.core.append(every(*[give(c, blk, 3) for c in range(2)]))
        second, third, corner = [], [], []
        for c in range(2):
            P, Q = orders[c]
            for jp in range(1, net.topo[P][0]):
                blk = net.block({0: k, P: jp})
                second += [wait(c, blk), give(c, blk, Q), give(c, blk, 3)]
                for jq in range(1, net.topo[Q][0]):
                    blk = net.block({0: k, P: jp, Q: jq})
                    corner += [wait(c, blk), give(c, blk, 3)]
            for jq in range(1, net.topo[Q][0]):
                blk = net.block({0: k, Q: jq})
                third += [wait(c, blk), give(c, blk, 3)]
        plan.second.append(every(*second))
        plan.third.append(every(*third))
        plan.corner.append(every(*corner))
    plan.rest = every(*[
        wait(c, net.block({0: k, 1: a, 2: b, 3: w}))
        for k in range(nz) for a in range(n1) for b in range(n2) for w in range(1, nc) for c in range(2)])
    return plan


def wait_sends(buf, send, blocks):
    ref = buf.at[pl.ds(0, blocks)]
    pltpu.make_async_copy(ref, ref, send).wait()


def scatter_events(net, G, RB, send, recv):
    RP = G.shape[1]
    cut = halves(RP)
    nz, n1, n2, nc = [size for size, _ in net.topo]
    orders = ((2, 1), (1, 2))
    pending = []

    def flush():
        for start in pending:
            start()
        del pending[:]

    def rows(c):
        return pl.ds(cut[c][0], cut[c][1])

    def add(ref, blk, c):
        G[blk, rows(c), :] = G[blk, rows(c), :] + ref[...]

    def place(off, axis):
        return net.partner(axis, off[axis])

    def core_sum(off):
        blk = net.block(off)
        s = (place(off, 0) * n1 + place(off, 1)) * n2 + place(off, 2)
        sends = []
        for c in range(2):
            Q, P = orders[c]
            by = off[Q]
            if by:
                spot = place(off, 0) * net.topo[P][0] + place(off, P)
                peer = net.move(net.me, Q, by)
                sends.append((c, by - 1, spot, peer))

        def run():
            for w in range(1, nc):
                remote(RB[0].at[w - 1, s], RB[0].at[w - 1, s], send, recv[0].at[w - 1, s], net.me).wait_recv()
            for c in range(2):
                for w in range(1, nc):
                    add(RB[0].at[w - 1, s, rows(c), :], blk, c)
            flush()
            for c, by, spot, peer in sends:
                pending.append(lambda c=c, by=by, spot=spot, peer=peer: remote(
                    G.at[blk, rows(c), :], RB[1][c].at[by, spot], send, recv[1][c].at[by, spot], peer).start())

        return run

    def second(c, off):
        Q, P = orders[c]
        blk = net.block(off)
        at_z = place(off, 0)
        spot = at_z * net.topo[P][0] + place(off, P)
        by = off[P]
        peer = net.move(net.me, P, by)

        def run():
            for j in range(net.topo[Q][0] - 1):
                ref = RB[1][c].at[j, spot]
                remote(ref, ref, send, recv[1][c].at[j, spot], net.me).wait_recv()
                add(ref, blk, c)
            flush()
            if by:
                pending.append(lambda: remote(
                    G.at[blk, rows(c), :], RB[2][c].at[by - 1, at_z], send, recv[2][c].at[by - 1, at_z], peer).start())

        return run

    def third(c, off):
        Q, P = orders[c]
        blk = net.block(off)
        at_z = place(off, 0)
        by = off[0]
        peer = net.move(net.me, 0, by)

        def run():
            for j in range(net.topo[P][0] - 1):
                ref = RB[2][c].at[j, at_z]
                remote(ref, ref, send, recv[2][c].at[j, at_z], net.me).wait_recv()
                add(ref, blk, c)
            flush()
            if by:
                pending.append(lambda: remote(
                    G.at[blk, rows(c), :], RB[3][c].at[by - 1], send, recv[3][c].at[by - 1], peer).start())

        return run

    def last():
        flush()
        for c in range(2):
            for by in range(1, nz):
                ref = RB[3][c].at[by - 1]
                remote(ref, ref, send, recv[3][c].at[by - 1], net.me).wait_recv()

    events = []
    z_order = [k for k in range(1, nz)] + [0]
    plane = sorted(((a, b) for a in range(n1) for b in range(n2)), key=lambda ab: -((ab[0] > 0) + (ab[1] > 0)))
    for r, k in enumerate(z_order):
        for a, b in plane:
            events.append((r, core_sum({0: k, 1: a, 2: b})))
        for c in range(2):
            Q, P = orders[c]
            for j in list(range(1, net.topo[P][0])) + [0]:
                events.append((r + 1.5 + 0.1 * (j == 0), second(c, {0: k, P: j, Q: 0})))
            events.append((r + 2.7, third(c, {0: k, P: 0, Q: 0})))
    events.sort(key=lambda e: e[0])
    return [e[1] for e in events] + [last], flush


def pack_and_send(net, S, G, RB, send, recv, nd, rows):
    nz, n1, n2, nc = [size for size, _ in net.topo]
    F = S.F

    def chip(t):
        a = lax.div(t, n1 * n2)
        b = lax.rem(lax.div(t, n2), n1)
        g = lax.rem(t, n2)
        base = a * net.topo[0][1] + b * net.topo[1][1] + g * net.topo[2][1]
        return base

    def pack(blk):
        G[blk, 0:rows, :] = F[pl.ds(rows * blk, rows), :].astype(bf)

    def go(t, w):
        blk = chip(t) + lax.rem(net.at[3] + w, nc) * net.topo[3][1]
        remote(G.at[blk], RB[0].at[w - 1, t], send, recv[0].at[w - 1, t], net.move(net.me, 3, w)).start()

    total = nz * n1 * n2
    for w in range(1, nc):
        def step(t, c):
            pack(chip(t) + lax.rem(net.at[3] + w, nc) * net.topo[3][1])

            @pl.when(t > 0)
            def _():
                go(t - 1, w)

            return c

        lax.fori_loop(0, total, step, 0)

    def mine(t, c):
        pack(chip(t) + net.at[3] * net.topo[3][1])
        return c

    lax.fori_loop(0, total, mine, 0)
    for w in range(1, nc):
        go(total - 1, w)


def spread(events, points):
    n = len(events)
    return [events[n * p // points : n * (p + 1) // points] for p in range(points)]


def at_points(groups, index, flush):
    for value, group in enumerate(groups):
        if group:

            @pl.when(index == value)
            def _(group=group):
                for event in group:
                    event()
                flush()


def kernel(cfg, counts, images, cotangent, master, act, dimg, o_grad, *scr):
    topo, L, NI, nd, rows, slots = cfg
    S = NS()
    for name, ref in zip(NAMES, scr):
        setattr(S, name, ref)
    S.wg = S.wgs
    net = Net(topo)
    nz = topo[0][0]

    barrier = pltpu.get_barrier_semaphore()
    peers = net.peers()
    for peer in peers:
        pl.semaphore_signal(barrier, inc=1, device_id=(peer,), device_id_type=pl.DeviceIdType.MESH)

    loads = [
        pltpu.make_async_copy(master, S.vm, S.lsem.at[0]),
        pltpu.make_async_copy(images, S.vimg, S.lsem.at[1]),
        pltpu.make_async_copy(cotangent, S.vcot, S.lsem.at[2]),
    ]
    for load in loads:
        load.start()
    loads[0].wait()
    for l in range(L):
        S.wg[l, net.me, 0:rows, :] = S.vm[:, l, :].astype(bf)
    pl.semaphore_wait(barrier, len(peers))

    gathers = [gather_plan(net, S.wg.at[l], S.gsend.at[l], S.grecv.at[l]) for l in range(L)]
    now = gathers[0]
    now.along()
    now.near[0]()
    now.far[0]()
    now.core[0]()

    def live(m, s):
        return s < counts[0, m]

    loads[1].wait()
    loads[2].wait()
    edge = SEQ - SEQ % 16

    def init(m, c):
        S.vdx[m] = S.vimg[m].astype(f32)
        for s in range(slots):
            i = m * slots + s
            S.X[i, edge:, :] = jnp.zeros((TP - edge, D), f32)
            S.DX[i, edge:, :] = jnp.zeros((TP - edge, D), f32)
            S.X[i, 0:SEQ, :] = S.vdx[m, :, s, :]
            for l in range(L):
                S.Q[l, i, TP:, :] = jnp.zeros((QP - TP, D), bf)
        S.vdx[m] = S.vcot[m].astype(f32)
        for s in range(slots):
            S.DX[m * slots + s, 0:SEQ, :] = jnp.where(live(m, s), S.vdx[m, :, s, :], 0.0)
        return c

    lax.fori_loop(0, NI // slots, init, 0)
    S.DO[TP:, :] = jnp.zeros((QP - TP, D), bf)

    steps = []
    for k in range(nz):
        at = 3.4 * k
        if k:
            steps += [(at, now.land[k]), (at, now.near[k]), (at, now.far[k]), (at, now.core[k])]
        steps += [(at + 3.3, now.second[k]), (at + 4.5, now.third[k]), (at + 7.5, now.corner[k])]
    steps.append((3.4 * (nz - 1) + 0.1, lambda: [g.along() for g in gathers[1:2]]))
    steps.append((3.4 * (nz - 1) + 3.4, lambda: [part() for g in gathers[1:2] for part in (g.near[0], g.far[0], g.core[0])]))
    for _, step in sorted(steps, key=lambda e: e[0]):
        step()
    now.rest()
    unpack_layer(S, 0, nd, rows)

    def nothing():
        pass

    for l in range(L):
        groups = [[] for _ in range(2 * NI)]
        if l + 1 < L:
            g = gathers[l + 1]
            if l:
                g.along()
                g.near[0]()
                g.far[0]()
                g.core[0]()
            for k in range(1, nz):
                g.land[k]()
                g.near[k]()
            for part in (g.far, g.core):
                for k in range(1, nz):
                    part[k]()
            g.second[0]()
            late = [(1.6 + 1.4 * k, g.second[k]) for k in range(1, nz)]
            late += [(4.8 + 1.4 * k, g.third[k]) for k in range(nz)]
            late += [(9.8 + 1.4 * k, g.corner[k]) for k in range(nz)]
            for at, step in sorted(late, key=lambda e: e[0]):
                groups[min(max(int(at / 1.6) - 1, 0), 2 * NI - 1)].append(step)

        def forward(i, c):
            fwd_attention(S, l, i)
            at_points(groups[0::2], i, nothing)
            fwd_mlp(S, l, i)
            at_points(groups[1::2], i, nothing)
            return c

        lax.fori_loop(0, NI, forward, 0)
        if l + 1 < L:
            g.rest()
            unpack_layer(S, l + 1, nd, rows)

    for l in range(L):
        wait_sends(S.wg.at[l], S.gsend.at[l], nd - 1)

    S.F[R_END:, :] = jnp.zeros((nd * rows - R_END, 128), f32)
    RB = [S.rb0, [S.rb1a, S.rb1b], [S.rb2a, S.rb2b], [S.rb3a, S.rb3b]]

    def recv_of(l):
        return [S.rr0.at[l], [S.rr1.at[l, c] for c in range(2)], [S.rr2.at[l, c] for c in range(2)], [S.rr3.at[l, c] for c in range(2)]]

    def total(l):
        wait_sends(S.wg.at[l], S.rsend.at[l], nd - 1)
        g = []
        for c, (first, count) in enumerate(halves(S.wg.shape[2])):
            part = S.wg[l, net.me, pl.ds(first, count), :].astype(f32)
            for by in range(nz - 1):
                part = part + RB[3][c][by].astype(f32)
            g.append(part)
        S.vm[:, l, :] = jnp.concatenate(g, axis=0)[0:rows]

    pend, flush = [], nothing
    for l in reversed(range(L)):
        groups = spread(pend[:-1], 2 * NI)
        S.VG[...] = jnp.zeros_like(S.VG)

        def backward(i, c):
            bwd_mlp(S, l, i)
            at_points(groups[0::2], i, flush)
            bwd_attention(S, l, i)
            at_points(groups[1::2], i, flush)
            return c

        lax.fori_loop(0, NI, backward, 0)
        grads_mlp(S, l)
        grads_attention(S, l)
        if l + 1 < L:
            pend[-1]()
            total(l + 1)
            for peer in peers:
                pl.semaphore_signal(S.credit, inc=1, device_id=(peer,), device_id_type=pl.DeviceIdType.MESH)
            pl.semaphore_wait(S.credit, len(peers))
        recv = recv_of(l)
        pack_and_send(net, S, S.wg.at[l], RB, S.rsend.at[l], recv, nd, rows)
        pend, flush = scatter_events(net, S.wg.at[l], RB, S.rsend.at[l], recv)

    def out_tokens(m, c):
        for s in range(slots):
            S.vdx[m, :, s, :] = jnp.where(live(m, s), S.X[m * slots + s, 0:SEQ, :], 0.0)
        S.vimg[m] = S.vdx[m].astype(bf)
        for s in range(slots):
            S.vdx[m, :, s, :] = S.DX[m * slots + s, 0:SEQ, :]
        return c

    lax.fori_loop(0, NI // slots, out_tokens, 0)
    outs = [pltpu.make_async_copy(S.vimg, act, S.lsem.at[1]), pltpu.make_async_copy(S.vdx, dimg, S.lsem.at[2])]
    for out in outs:
        out.start()
    for event in pend:
        event()
    total(0)
    outs.append(pltpu.make_async_copy(S.vm, o_grad, S.lsem.at[0]))
    outs[-1].start()
    for out in outs:
        out.wait()


NAMES = (
    ["Wq", "Wp", "Wu", "Wd", "V", "VG", "F", "X", "DX", "DO", "DM", "DA", "DQKV", "wgs"]
    + [name for name, _, _ in SAVED]
    + ["rb0", "rb1a", "rb1b", "rb2a", "rb2b", "rb3a", "rb3b"]
    + ["vm", "vimg", "vcot", "vdx"]
    + ["lsem", "gsend", "grecv", "rsend", "rr0", "rr1", "rr2", "rr3", "credit"]
)


def body(topo, images, cotangent, counts, master, moment_one, moment_two):
    micro, slots = images.shape[:2]
    NI = micro * slots
    L, width = master.shape
    rows = width // 128
    RP = 16 * ((rows + 15) // 16)
    nd = lax.axis_size("fsdp")
    (nz, _), (n1, _), (n2, _), (nc, _) = topo
    cut = halves(RP)

    VM, DMA = pltpu.VMEM, pltpu.SemaphoreType.DMA
    scratch = [
        VM((L, D, 3 * D), bf),
        VM((L, D, D), bf),
        VM((L, D, FF), bf),
        VM((L, FF, D), bf),
        VM((L, 16, FF), f32),
        VM((16, FF), f32),
        VM((nd * rows, 128), f32),
        VM((NI, TP, D), f32),
        VM((NI, TP, D), f32),
        VM((QP, D), bf),
        VM((NI, TP, D), bf),
        VM((NI, TP, D), bf),
        VM((NI, TP, 3 * D), bf),
        VM((L, nd, RP, 128), bf),
    ]
    scratch += [VM((L, NI) + shape, kind) for _, shape, kind in SAVED]
    scratch += [VM((max(nc - 1, 1), nz * n1 * n2, RP, 128), bf)]
    scratch += [
        VM((n2 - 1, nz * n1, cut[0][1], 128), bf),
        VM((n1 - 1, nz * n2, cut[1][1], 128), bf),
        VM((n1 - 1, nz, cut[0][1], 128), bf),
        VM((n2 - 1, nz, cut[1][1], 128), bf),
        VM((nz - 1, cut[0][1], 128), bf),
        VM((nz - 1, cut[1][1], 128), bf),
    ]
    tokens = (micro, SEQ, slots, D)
    scratch += [VM((rows, L, 128), f32), VM(tokens, bf), VM(tokens, bf), VM(tokens, f32)]
    wide_first = max(n1, n2) - 1
    scratch += [
        DMA((3,)),
        DMA((L,)),
        DMA((L, 2, nd)),
        DMA((L,)),
        DMA((L, max(nc - 1, 1), nz * n1 * n2)),
        DMA((L, 2, wide_first, nz * max(n1, n2))),
        DMA((L, 2, wide_first, nz)),
        DMA((L, 2, nz - 1)),
        pltpu.SemaphoreType.REGULAR,
    ]
    anywhere = pl.BlockSpec(memory_space=pl.ANY)
    act, grad_in, grad = pl.pallas_call(
        functools.partial(kernel, (topo, L, NI, nd, rows, slots)),
        out_shape=(
            jax.ShapeDtypeStruct(tokens, bf),
            jax.ShapeDtypeStruct(tokens, f32),
            jax.ShapeDtypeStruct((rows, L, 128), f32),
        ),
        in_specs=[pl.BlockSpec(memory_space=pltpu.SMEM)] + [anywhere] * 3,
        out_specs=(anywhere,) * 3,
        scratch_shapes=scratch,
        compiler_params=pltpu.CompilerParams(vmem_limit_bytes=67043328, collective_id=0, has_side_effects=True),
        name="step",
    )(
        counts.T,
        images.transpose(0, 2, 1, 3),
        cotangent.transpose(0, 2, 1, 3),
        master.reshape(L, rows, 128).transpose(1, 0, 2),
    )
    weight_grad = grad.transpose(1, 0, 2).reshape(L, width) / (NI * nd)
    first_new = beta_one * moment_one + (1.0 - beta_one) * weight_grad
    second_new = beta_two * moment_two + (1.0 - beta_two) * weight_grad * weight_grad
    update = first_new / (1.0 - beta_one**STEP) / (jnp.sqrt(second_new / (1.0 - beta_two**STEP)) + epsilon)
    new_master = master - learn_rate * (update + decay_rate * master)
    return (
        act.transpose(0, 2, 1, 3),
        grad_in.transpose(0, 2, 1, 3),
        weight_grad,
        new_master,
        first_new,
        second_new,
    )


def solution(mesh):
    topo = topology(mesh)
    tokens = P(None, "fsdp", None, None)
    state = P(None, "fsdp")
    return jax.shard_map(
        functools.partial(body, topo),
        mesh=mesh,
        in_specs=(tokens, tokens, state, state, state, state),
        out_specs=(tokens, tokens, state, state, state, state),
        check_vma=False,
    )
```

```python
import functools
import math

import jax
import jax.numpy as jnp
from jax import lax
from jax.experimental import pallas as pl
from jax.experimental.pallas import tpu as pltpu
from jax.sharding import PartitionSpec as P

D = 384
H = 6
HD = 64
FF = 1536
SEQ = 197
STEP = 3
TP = 208
QP = 256

beta_one = 0.9
beta_two = 0.999
learn_rate = 0.05
decay_rate = 0.05
epsilon = 1e-08

f32 = jnp.float32
bf = jnp.bfloat16
R_QKV, R_P, R_U, R_D, R_END = 36, 3492, 4644, 9252, 13860
NN = (((1,), (0,)), ((), ()))
NT = (((1,), (1,)), ((), ()))
TN = (((0,), (0,)), ((), ()))
G1, B1, BQ, BV, BP, G2, B2, BD, BU = range(9)


def dot(a, b, dims):
    return lax.dot_general(a, b, dims, preferred_element_type=f32)


def wide(r):
    return jnp.concatenate([r, r, r], axis=1)


def rowsum(x):
    return jnp.sum(x, 0, keepdims=True)


def norm(x):
    m = jnp.sum(x, -1, keepdims=True) * (1.0 / D)
    c = x - m
    v = jnp.sum(c * c, -1, keepdims=True) * (1.0 / D)
    r = lax.rsqrt(v + 1e-6)
    return c * r, jnp.broadcast_to(r, (x.shape[0], 128))


def norm_back(dh, n, r, g, dy):
    e = dh * g
    me = jnp.sum(e, -1, keepdims=True) * (1.0 / D)
    men = jnp.sum(e * n, -1, keepdims=True) * (1.0 / D)
    return dy + (e - me - n * men) * wide(r)


def half_mask(rows, e):
    lane = lax.broadcasted_iota(jnp.int32, (rows, 128), 1)
    return (lane < 64) if e == 0 else (lane >= 64)


def keep(mask, v):
    return jnp.where(mask, v, jnp.zeros_like(v))


class NS:
    pass


SAVED = [
    ("N1", (TP, D), bf),
    ("R1", (TP, 128), f32),
    ("Q", (QP, D), bf),
    ("KV", (TP, 2 * D), bf),
    ("PT", (H, TP, QP), bf),
    ("O", (TP, D), bf),
    ("N2", (TP, D), bf),
    ("R2", (TP, 128), f32),
    ("GB", (TP, FF), bf),
    ("GP", (TP, FF), bf),
]


def unpack_layer(S, l, nd, rows):
    wg, F, V = S.wg.at[l], S.F, S.V.at[l]

    def put(d, c):
        F[pl.ds(rows * d, rows), :] = wg[d, 0:rows, :].astype(f32)
        return c

    lax.fori_loop(0, nd, put, 0)
    for k in range(8):
        for j in range(3):
            V[k : k + 1, 128 * j : 128 * j + 128] = F[3 * k + j : 3 * k + j + 1, :]
    for j in range(12):
        V[8:9, 128 * j : 128 * j + 128] = F[24 + j : 25 + j, :]
    for W, off, h, w in ((S.Wq, R_QKV, D, 3 * D), (S.Wp, R_P, D, D), (S.Wu, R_U, D, FF), (S.Wd, R_D, FF, D)):
        n = w // 128
        for j in range(n):
            W[l, :, 128 * j : 128 * j + 128] = F[pl.ds(off + j, h, stride=n), :].astype(bf)


def fwd_attention(S, l, i):
    V = S.V
    n1, r1 = norm(S.X[i])
    S.N1[l, i] = n1.astype(bf)
    S.R1[l, i] = r1
    h = (n1 * V[l, G1 : G1 + 1, 0:D] + V[l, B1 : B1 + 1, 0:D]).astype(bf)
    qkv = dot(h, S.Wq[l], NN)
    S.Q[l, i, 0:TP, :] = (qkv[:, 0:D] + V[l, BQ : BQ + 1, 0:D]).astype(bf)
    S.KV[l, i, :, 0:D] = qkv[:, D : 2 * D].astype(bf)
    S.KV[l, i, :, D : 2 * D] = (qkv[:, 2 * D :] + V[l, BV : BV + 1, 0:D]).astype(bf)
    row = lax.broadcasted_iota(jnp.int32, (TP, QP), 0)
    for p in range(3):
        kp = S.KV[l, i, :, 128 * p : 128 * p + 128] * jnp.asarray(0.125, bf)
        vp = S.KV[l, i, :, D + 128 * p : D + 128 * p + 128]
        qp = S.Q[l, i, :, 128 * p : 128 * p + 128]
        o = None
        for e in range(2):
            m = half_mask(TP, e)
            s = dot(keep(m, kp), qp, NT)
            s = jnp.where(row < SEQ, s, -1e30)
            ex = jnp.exp(s - jnp.max(s, 0, keepdims=True))
            pb = (ex * (1.0 / jnp.sum(ex, 0, keepdims=True))).astype(bf)
            S.PT[l, i, 2 * p + e] = pb
            oo = dot(pb, keep(m, vp), TN)
            o = oo if o is None else o + oo
        S.O[l, i, :, 128 * p : 128 * p + 128] = o[0:TP].astype(bf)


def fwd_mlp(S, l, i):
    V = S.V
    x1 = S.X[i] + dot(S.O[l, i], S.Wp[l], NN) + V[l, BP : BP + 1, 0:D]
    n2, r2 = norm(x1)
    S.N2[l, i] = n2.astype(bf)
    S.R2[l, i] = r2
    h2 = (n2 * V[l, G2 : G2 + 1, 0:D] + V[l, B2 : B2 + 1, 0:D]).astype(bf)
    for c in range(3):
        sl = slice(512 * c, 512 * c + 512)
        u = dot(h2, S.Wu[l, :, sl], NN) + V[l, BU : BU + 1, sl]
        phi = 0.5 + 0.5 * lax.erf(u * math.sqrt(0.5))
        S.GB[l, i, :, sl] = (u * phi).astype(bf)
        S.GP[l, i, :, sl] = (phi + u * (jnp.exp(u * u * -0.5) * (1.0 / math.sqrt(2 * math.pi)))).astype(bf)
    S.X[i] = x1 + dot(S.GB[l, i], S.Wd[l], NN) + V[l, BD : BD + 1, 0:D]


def bwd_mlp(S, l, i):
    V, VG = S.V, S.VG
    dy = S.DX[i]
    dm = dy.astype(bf)
    S.DM[i] = dm
    VG[BD : BD + 1, 0:D] += rowsum(dy)
    for c in range(3):
        sl = slice(512 * c, 512 * c + 512)
        du = dot(dm, S.Wd[l, sl, :], NT) * S.GP[l, i, :, sl].astype(f32)
        VG[BU : BU + 1, sl] += rowsum(du)
        S.GP[l, i, :, sl] = du.astype(bf)
    dh2 = dot(S.GP[l, i], S.Wu[l], NT)
    n2 = S.N2[l, i].astype(f32)
    VG[G2 : G2 + 1, 0:D] += rowsum(dh2 * n2)
    VG[B2 : B2 + 1, 0:D] += rowsum(dh2)
    dx1 = norm_back(dh2, n2, S.R2[l, i], V[l, G2 : G2 + 1, 0:D], dy)
    VG[BP : BP + 1, 0:D] += rowsum(dx1)
    S.DA[i] = dx1.astype(bf)
    S.DX[i] = dx1


def bwd_attention(S, l, i):
    V, VG = S.V, S.VG
    S.DO[0:TP, :] = dot(S.DA[i], S.Wp[l], NT).astype(bf)
    eighth = jnp.asarray(0.125, bf)
    for p in range(3):
        kp = S.KV[l, i, :, 128 * p : 128 * p + 128] * eighth
        vp = S.KV[l, i, :, D + 128 * p : D + 128 * p + 128]
        qp = S.Q[l, i, :, 128 * p : 128 * p + 128] * eighth
        do = S.DO[:, 128 * p : 128 * p + 128]
        dq = dk = dv = None
        for e in range(2):
            m = half_mask(TP, e)
            mq = half_mask(QP, e)
            pb = S.PT[l, i, 2 * p + e]
            dp = dot(keep(m, vp), do, NT)
            pf = pb.astype(f32)
            t = pf * dp
            ds = (t - pf * rowsum(t)).astype(bf)
            a = dot(pb, keep(mq, do), NN)
            b = dot(ds, keep(mq, qp), NN)
            c = dot(ds, keep(m, kp), TN)
            dv = a if dv is None else dv + a
            dk = b if dk is None else dk + b
            dq = c if dq is None else dq + c
        dq = dq[0:TP]
        sl = slice(128 * p, 128 * p + 128)
        VG[BQ : BQ + 1, sl] += rowsum(dq)
        VG[BV : BV + 1, sl] += rowsum(dv)
        S.DQKV[i, :, sl] = dq.astype(bf)
        S.DQKV[i, :, D + 128 * p : D + 128 * p + 128] = dk.astype(bf)
        S.DQKV[i, :, 2 * D + 128 * p : 2 * D + 128 * p + 128] = dv.astype(bf)
    dh = dot(S.DQKV[i], S.Wq[l], NT)
    n1 = S.N1[l, i].astype(f32)
    VG[G1 : G1 + 1, 0:D] += rowsum(dh * n1)
    VG[B1 : B1 + 1, 0:D] += rowsum(dh)
    S.DX[i] = norm_back(dh, n1, S.R1[l, i], V[l, G1 : G1 + 1, 0:D], S.DX[i])


def flat(v):
    return v.reshape(v.shape[0] * v.shape[1], v.shape[2])


def store_grad(F, val, first, n):
    for j in range(val.shape[1] // 128):
        F[pl.ds(first + j, val.shape[0], stride=n), :] = val[:, 128 * j : 128 * j + 128]


def grads_down(S, l):
    F = S.F
    dm = flat(S.DM[...])
    for c in range(3):
        gb = flat(S.GB[l, :, :, 512 * c : 512 * c + 512])
        store_grad(F, dot(gb, dm, TN), R_D + 3 * 512 * c, 3)


def grads_up(S, l):
    V, F = S.V, S.F
    h2 = (flat(S.N2[l]).astype(f32) * V[l, G2 : G2 + 1, 0:D] + V[l, B2 : B2 + 1, 0:D]).astype(bf)
    for c in range(3):
        du = flat(S.GP[l, :, :, 512 * c : 512 * c + 512])
        store_grad(F, dot(h2, du, TN), R_U + 4 * c, 12)


def grads_out(S, l):
    store_grad(S.F, dot(flat(S.O[l]), flat(S.DA[...]), TN), R_P, 3)


def grads_attention(S, l):
    V, VG, F = S.V, S.VG, S.F
    h = (flat(S.N1[l]).astype(f32) * V[l, G1 : G1 + 1, 0:D] + V[l, B1 : B1 + 1, 0:D]).astype(bf)
    for c0, c1 in ((0, 512), (512, 1024), (1024, 1152)):
        store_grad(F, dot(h, flat(S.DQKV[:, :, c0:c1]), TN), R_QKV + c0 // 128, 9)
    for k in range(8):
        for j in range(3):
            F[3 * k + j : 3 * k + j + 1, :] = VG[k : k + 1, 128 * j : 128 * j + 128]
    for j in range(12):
        F[24 + j : 25 + j, :] = VG[8:9, 128 * j : 128 * j + 128]


def topology(mesh):
    devices = list(mesh.devices.flat)
    where = {}
    for index, device in enumerate(devices):
        where[tuple(device.coords) + (device.core_on_chip,)] = index
    sizes = [max(key[a] for key in where) - min(key[a] for key in where) + 1 for a in range(4)]
    origin = [min(key[a] for key in where) for a in range(4)]
    dims = []
    for a in range(4):
        if sizes[a] > 1:
            step = list(origin)
            step[a] += 1
            dims.append((int(sizes[a]), int(where[tuple(step)] - where[tuple(origin)])))
        else:
            dims.append((1, 1))
    for key, index in where.items():
        assert index == sum((key[a] - origin[a]) * dims[a][1] for a in range(4))
    chip = sorted(dims[:3], key=lambda d: -d[0])
    return tuple(chip) + (dims[3],)


class Net:
    def __init__(self, topo):
        self.topo = topo
        self.me = lax.axis_index("fsdp")
        self.at = [lax.rem(lax.div(self.me, stride), size) for size, stride in topo]

    def move(self, index, axis, by):
        if by == 0 or self.topo[axis][0] == 1:
            return index
        return index + (self.partner(axis, by) - self.at[axis]) * self.topo[axis][1]

    def partner(self, axis, by):
        at, out, weight, size = self.at[axis], 0, 1, self.topo[axis][0]
        assert size & (size - 1) == 0
        while weight < size:
            bit = lax.rem(lax.div(at, weight), 2)
            out = out + weight * (1 - bit if by & weight else bit)
            weight *= 2
        return out

    def block(self, offsets):
        index = self.me
        for axis, by in offsets.items():
            index = self.move(index, axis, by)
        return index

    def peers(self):
        out = []
        for axis, (size, _) in enumerate(self.topo):
            out += [self.move(self.me, axis, by) for by in range(1, size)]
        return out


def remote(src, dst, send, recv, peer):
    return pltpu.make_async_remote_copy(
        src_ref=src, dst_ref=dst, send_sem=send, recv_sem=recv, device_id=(peer,), device_id_type=pl.DeviceIdType.MESH
    )


PARTS = 4


def parts(RP):
    tiles = RP // 16
    ends = [16 * (tiles * p // PARTS) for p in range(PARTS + 1)]
    return [(ends[p], ends[p + 1] - ends[p]) for p in range(PARTS)]


def gather_plan(net, wg, send, recv):
    RP = wg.shape[1]
    cut = parts(RP)
    nz, n1, n2, nc = [size for size, _ in net.topo]
    orders = ((1, 2), (2, 1)) * (PARTS // 2)
    plan = NS()

    def copy(c, blk, peer):
        first, count = cut[c]
        ref = wg.at[blk, pl.ds(first, count), :]
        return remote(ref, ref, send, recv.at[c, blk], peer)

    def wait(c, blk):
        return lambda: copy(c, blk, net.me).wait_recv()

    def give(c, blk, axis):
        ends = [net.move(net.me, axis, by) for by in range(1, net.topo[axis][0])]

        def run():
            for peer in ends:
                copy(c, blk, peer).start()

        return run

    def every(*steps):
        def run():
            for step in steps:
                step()

        return run

    plan.along = every(*[every(*[
        (lambda c=c, peer=peer: copy(c, net.me, peer).start()) for c in range(PARTS)]) for peer in [net.move(net.me, 0, by) for by in range(1, nz)]])
    plan.land, plan.near, plan.far, plan.core = [], [], [], []
    plan.second, plan.third, plan.corner = [], [], []
    for k in range(nz):
        blk = net.block({0: k})
        plan.land.append(every(*[wait(c, blk) for c in range(PARTS)]) if k else every())
        plan.near.append(every(*[give(c, blk, orders[c][0]) for c in range(PARTS)]))
        plan.far.append(every(*[give(c, blk, orders[c][1]) for c in range(PARTS)]))
        plan.core.append(every(*[give(c, blk, 3) for c in range(PARTS)]))
        second, third, corner = [], [], []
        for c in range(PARTS):
            P, Q = orders[c]
            for jp in range(1, net.topo[P][0]):
                blk = net.block({0: k, P: jp})
                second += [wait(c, blk), give(c, blk, Q), give(c, blk, 3)]
                for jq in range(1, net.topo[Q][0]):
                    blk = net.block({0: k, P: jp, Q: jq})
                    corner += [wait(c, blk), give(c, blk, 3)]
            for jq in range(1, net.topo[Q][0]):
                blk = net.block({0: k, Q: jq})
                third += [wait(c, blk), give(c, blk, 3)]
        plan.second.append(every(*second))
        plan.third.append(every(*third))
        plan.corner.append(every(*corner))
    plan.rest = every(*[
        wait(c, net.block({0: k, 1: a, 2: b, 3: w}))
        for k in range(nz) for a in range(n1) for b in range(n2) for w in range(1, nc) for c in range(PARTS)])
    return plan


def wait_sends(buf, send, blocks):
    ref = buf.at[pl.ds(0, blocks)]
    pltpu.make_async_copy(ref, ref, send).wait()


def run(events):
    def when(test, do):
        if do is None:
            return
        if test is None:
            do()
        else:
            pl.when(test)(do)

    previous = None
    for *_, take, take_if, give, give_if in events:
        when(take_if, take)
        if previous is not None:
            when(*previous)
        previous = (give_if, give)
    if previous is not None:
        when(*previous)


def both(*tests):
    out = None
    for test in tests:
        if test is not None:
            out = test if out is None else jnp.logical_and(out, test)
    return out


def scatter_plan(net, G, RB, send, recv, bounds, margin):
    RP = G.shape[1]
    cut = parts(RP)
    nz, n1, n2, nc = [size for size, _ in net.topo]
    orders = ((2, 1), (1, 2)) * (PARTS // 2)
    low = nz.bit_length() - 1

    def rows(c):
        return pl.ds(cut[c][0], cut[c][1])

    def add(ref, blk, c):
        G[blk, rows(c), :] = G[blk, rows(c), :] + ref[...]

    def bit(v, s):
        return lax.rem(lax.div(v, 1 << s), 2)

    def block(g, off):
        blk = net.block({axis: by for axis, by in off.items()})
        return blk + (g - net.at[0]) * net.topo[0][1]

    def core_sum(g, off):
        blk = block(g, off)
        spot = (g * n1 + net.partner(1, off[1])) * n2 + net.partner(2, off[2])
        sends = []
        for c in range(PARTS):
            Q, P = orders[c]
            if off[Q]:
                sends.append((c, off[Q] - 1, g * net.topo[P][0] + net.partner(P, off[P]), net.move(net.me, Q, off[Q])))

        def take():
            for w in range(1, nc):
                ref = RB[0].at[w - 1, spot]
                remote(ref, ref, send, recv[0].at[w - 1, spot], net.me).wait_recv()
            for w in range(1, nc):
                for c in range(PARTS):
                    add(RB[0].at[w - 1, spot, rows(c), :], blk, c)

        def give():
            for c, by, to, peer in sends:
                remote(G.at[blk, rows(c), :], RB[1][c].at[by, to], send, recv[1][c].at[by, to], peer).start()

        return take, None, give if sends else None, None

    def second(c, g, off):
        Q, P = orders[c]
        blk = block(g, off)
        spot = g * net.topo[P][0] + net.partner(P, off[P])
        by = off[P]
        peer = net.move(net.me, P, by)

        def take():
            for j in range(net.topo[Q][0] - 1):
                ref = RB[1][c].at[j, spot]
                remote(ref, ref, send, recv[1][c].at[j, spot], net.me).wait_recv()
                add(ref, blk, c)

        def give():
            remote(G.at[blk, rows(c), :], RB[2][c].at[by - 1, g], send, recv[2][c].at[by - 1, g], peer).start()

        return take, None, give if by else None, None

    def slot(g, s):
        return sum(nz >> (t + 1) for t in range(s)) + (g >> (s + 1))

    def along(c, g, s):
        blk = block(g, {1: 0, 2: 0})
        peer = net.move(net.me, 0, 1 << s)

        def give():
            at = slot(g, s)
            remote(G.at[blk, rows(c), :], RB[3][c].at[at], send, recv[3][c].at[at], peer).start()

        return give, (bit(net.at[0], s) != (g >> s) % 2)

    def third(c, g):
        Q, P = orders[c]
        blk = block(g, {1: 0, 2: 0})

        def take():
            for j in range(net.topo[P][0] - 1):
                ref = RB[2][c].at[j, g]
                remote(ref, ref, send, recv[2][c].at[j, g], net.me).wait_recv()
                add(ref, blk, c)

        return (take, None) + (along(c, g, 0) if low else (None, None))

    def halving(c, g, s):
        blk = block(g, {1: 0, 2: 0})
        same = lax.rem(net.at[0], 2 << s) == g % (2 << s)

        def take():
            at = slot(g, s)
            ref = RB[3][c].at[at]
            remote(ref, ref, send, recv[3][c].at[at], net.me).wait_recv()
            add(ref, blk, c)

        give, differs = along(c, g, s + 1)
        return take, same, give, jnp.logical_and(same, differs)

    def member(g, off, inside):
        if len(inside) == n1 * n2:
            return None
        a, b = net.partner(1, off[1]), net.partner(2, off[2])
        spot = a * n2 + b
        return both(spot >= inside[0], spot <= inside[-1])

    plane = sorted(((a, b) for a in range(n1) for b in range(n2)), key=lambda ab: -((ab[0] > 0) + (ab[1] > 0)))
    lists = []
    for w in range(len(bounds) - 1):
        events, n = [], 0
        hidden = w + 2 < len(bounds) or margin > 1.0
        slack = margin * hidden
        for g in reversed(range(nz)):
            inside = [t % (n1 * n2) for t in range(bounds[w + 1], bounds[w]) if t // (n1 * n2) == g]
            if not inside:
                continue

            def put(at, stage, event, off):
                take, take_if, give, give_if = event
                test = member(g, off, inside)
                events.append([at, stage, (id(G), w, g), take, both(test, take_if), give, both(test, give_if)])

            for r, (a, b) in enumerate(plane):
                put(1.2 + 0.5 * slack + 1.2 * n + 0.3 * r, 0, core_sum(g, {1: a, 2: b}), {1: a, 2: b})
            for c in range(PARTS):
                Q, P = orders[c]
                for j in list(range(1, net.topo[P][0])) + [0]:
                    off = {P: j, Q: 0}
                    put(4.0 + slack + 2.6 * n + 1.3 * (j == 0) + 0.1 * c, 1 + (j == 0), second(c, g, off), off)
                after = max(6.8 + 2.6 * n, (10.8 + 1.3 * n) * hidden) + slack + 0.1 * c
                put(after, 3, third(c, g), {1: 0, 2: 0})
                for s in range(low - 1):
                    put(after + 2.5 * (s + 1) + (7.5 if margin > 1.0 else 4.0) * hidden, 4 + s, halving(c, g, s), {1: 0, 2: 0})
            n += 1
        lists.append(sorted(events, key=lambda e: e[0]))
    return lists


def pack_and_send(net, S, G, RB, send, recv, nd, rows, chips):
    nz, n1, n2, nc = [size for size, _ in net.topo]
    F = S.F
    first, last = chips

    def block(t, w):
        base = lax.div(t, n1 * n2) * net.topo[0][1] + lax.rem(lax.div(t, n2), n1) * net.topo[1][1] + lax.rem(t, n2) * net.topo[2][1]
        core = net.at[3] if w == 0 else net.partner(3, w)
        return base + core * net.topo[3][1]

    def pack(blk):
        G[blk, 0:rows, :] = F[pl.ds(rows * blk, rows), :].astype(bf)

    def go(t, w):
        remote(G.at[block(t, w)], RB[0].at[w - 1, t], send, recv[0].at[w - 1, t], net.move(net.me, 3, w)).start()

    for w in range(1, nc):

        def step(k, c):
            t = last - 1 - k
            pack(block(t, w))

            @pl.when(k > 0)
            def _():
                go(t + 1, w)

            return c

        lax.fori_loop(0, last - first, step, 0)

    def mine(k, c):
        pack(block(last - 1 - k, 0))
        return c

    lax.fori_loop(0, last - first, mine, 0)
    for w in range(1, nc):
        go(first, w)


def chips_before(topo, rows, row):
    (nz, sz), (n1, s1), (n2, s2), _ = topo
    count = 0
    for t in range(nz * n1 * n2):
        base = (t // (n1 * n2)) * sz + (t // n2 % n1) * s1 + (t % n2) * s2
        if rows * base < row:
            count = t + 1
    return count


AFTER = [0.0, 2.4, 3.4, 4.8, 7.4] + [10.4 + 3.0 * k for k in range(8)]


def at_points(groups, index):
    for value, group in enumerate(groups):
        if group:

            @pl.when(index == value)
            def _(group=group):
                run(group)


def kernel(cfg, counts, images, cotangent, master, act, dimg, o_grad, *scr):
    topo, L, NI, nd, rows, slots = cfg
    S = NS()
    for name, ref in zip(NAMES, scr):
        setattr(S, name, ref)
    S.wg = S.wgs
    net = Net(topo)
    nz = topo[0][0]

    barrier = pltpu.get_barrier_semaphore()
    peers = net.peers()
    for peer in peers:
        pl.semaphore_signal(barrier, inc=1, device_id=(peer,), device_id_type=pl.DeviceIdType.MESH)

    loads = [
        pltpu.make_async_copy(master, S.vm, S.lsem.at[0]),
        pltpu.make_async_copy(images, S.vimg, S.lsem.at[1]),
        pltpu.make_async_copy(cotangent, S.vcot, S.lsem.at[2]),
    ]
    for load in loads:
        load.start()
    loads[0].wait()
    for l in range(L):
        S.wg[l, net.me, 0:rows, :] = S.vm[:, l, :].astype(bf)
    pl.semaphore_wait(barrier, len(peers))

    gathers = [gather_plan(net, S.wg.at[l], S.gsend.at[l], S.grecv.at[l]) for l in range(L)]
    now = gathers[0]
    now.along()
    now.near[0]()
    now.far[0]()
    now.core[0]()

    def live(m, s):
        return s < counts[0, m]

    loads[1].wait()
    loads[2].wait()
    edge = SEQ - SEQ % 16

    def init(m, c):
        S.vdx[m] = S.vimg[m].astype(f32)
        for s in range(slots):
            i = m * slots + s
            S.X[i, edge:, :] = jnp.zeros((TP - edge, D), f32)
            S.DX[i, edge:, :] = jnp.zeros((TP - edge, D), f32)
            S.X[i, 0:SEQ, :] = S.vdx[m, :, s, :]
            for l in range(L):
                S.Q[l, i, TP:, :] = jnp.zeros((QP - TP, D), bf)
        S.vdx[m] = S.vcot[m].astype(f32)
        for s in range(slots):
            S.DX[m * slots + s, 0:SEQ, :] = jnp.where(live(m, s), S.vdx[m, :, s, :], 0.0)
        return c

    lax.fori_loop(0, NI // slots, init, 0)
    S.DO[TP:, :] = jnp.zeros((QP - TP, D), bf)

    steps = []
    for k in range(nz):
        at = 3.4 * k
        if k:
            steps += [(at, now.land[k]), (at, now.near[k]), (at, now.far[k]), (at, now.core[k])]
        steps += [(at + 3.3, now.second[k]), (at + 4.5, now.third[k]), (at + 7.5, now.corner[k])]
    steps.append((3.4 * (nz - 1) + 0.1, lambda: [g.along() for g in gathers[1:2]]))
    steps.append((3.4 * (nz - 1) + 3.4, lambda: [part() for g in gathers[1:2] for part in (g.near[0], g.far[0], g.core[0])]))
    for _, step in sorted(steps, key=lambda e: e[0]):
        step()
    now.rest()
    unpack_layer(S, 0, nd, rows)

    for l in range(L):
        groups = [[] for _ in range(2 * NI)]
        if l + 1 < L:
            g = gathers[l + 1]
            if l:
                g.along()
                g.near[0]()
                g.far[0]()
                g.core[0]()
            for k in range(1, nz):
                g.land[k]()
                g.near[k]()
            for part in (g.far, g.core):
                for k in range(1, nz):
                    part[k]()
            g.second[0]()
            late = [(1.6 + 1.4 * k, g.second[k]) for k in range(1, nz)]
            late += [(4.8 + 1.4 * k, g.third[k]) for k in range(nz)]
            late += [(9.8 + 1.4 * k, g.corner[k]) for k in range(nz)]
            for at, step in sorted(late, key=lambda e: e[0]):
                groups[min(max(int(at / 1.6) - 1, 0), 2 * NI - 1)].append((step, None, None, None))

        def forward(i, c):
            fwd_attention(S, l, i)
            at_points(groups[0::2], i)
            fwd_mlp(S, l, i)
            at_points(groups[1::2], i)
            return c

        lax.fori_loop(0, NI, forward, 0)
        if l + 1 < L:
            g.rest()
            unpack_layer(S, l + 1, nd, rows)

    for l in range(L):
        wait_sends(S.wg.at[l], S.gsend.at[l], nd - 1)

    S.F[R_END:, :] = jnp.zeros((nd * rows - R_END, 128), f32)
    RB = [
        [S.rb0.at[l]] + [[getattr(S, "rb%d_%d" % (stage, c)).at[l] for c in range(PARTS)] for stage in (1, 2, 3)]
        for l in range(L)
    ]
    recvs = [
        [S.rr0.at[l]] + [[ref.at[l, c] for c in range(PARTS)] for ref in (S.rr1, S.rr2, S.rr3)] for l in range(L)
    ]
    bounds = [nz * topo[1][0] * topo[2][0], chips_before(topo, rows, R_D), chips_before(topo, rows, R_P), 0]
    plans = [scatter_plan(net, S.wg.at[l], RB[l], S.rsend.at[l], recvs[l], bounds, 1.2 if l else 0.3) for l in range(L)]

    def total(l):
        for c in range(PARTS):
            if nz > 1:
                ref = RB[l][3][c].at[nz - 2]
                remote(ref, ref, S.rsend.at[l], recvs[l][3][c].at[nz - 2], net.me).wait_recv()
        wait_sends(S.wg.at[l], S.rsend.at[l], nd - 1)
        g = []
        for c, (first, count) in enumerate(parts(S.wg.shape[2])):
            part = S.wg[l, net.me, pl.ds(first, count), :].astype(f32)
            if nz > 1:
                part = part + RB[l][3][c][nz - 2].astype(f32)
            g.append(part)
        S.vm[:, l, :] = jnp.concatenate(g, axis=0)[0:rows]

    queue = []
    clock = [0.0]

    def add_events(events):
        queue.extend([clock[0] + event[0]] + event[1:] for event in events)
        queue.sort(key=lambda event: event[0])

    def due(passed):
        clock[0] += passed
        events = []
        while queue and queue[0][0] <= clock[0]:
            event = queue.pop(0)
            events.append(event)
            for other in queue:
                if other[2] == event[2] and other[1] > event[1]:
                    other[0] = max(other[0], clock[0] + AFTER[other[1]] - AFTER[event[1]])
            queue.sort(key=lambda other: other[0])
        return events

    def ship(l, w):
        chips = bounds[w + 1], bounds[w]
        if chips[0] < chips[1]:
            pack_and_send(net, S, S.wg.at[l], RB[l], S.rsend.at[l], recvs[l], nd, rows, chips)
            add_events(plans[l][w])

    for l in reversed(range(L)):
        S.VG[...] = jnp.zeros_like(S.VG)
        groups = [due(1.15) for _ in range(NI)]

        def backward_mlp(i, c):
            bwd_mlp(S, l, i)
            at_points(groups, i)
            return c

        lax.fori_loop(0, NI, backward_mlp, 0)
        grads_down(S, l)
        ship(l, 0)
        run(due(1.8))
        grads_up(S, l)
        run(due(1.5))
        grads_out(S, l)
        ship(l, 1)
        run(due(1.3))
        groups = [due(2.15) for _ in range(NI)]

        def backward_attention(i, c):
            bwd_attention(S, l, i)
            at_points(groups, i)
            return c

        lax.fori_loop(0, NI, backward_attention, 0)
        grads_attention(S, l)
        ship(l, 2)
        run(due(1.6))

    def out_tokens(m, c):
        for s in range(slots):
            S.vdx[m, :, s, :] = jnp.where(live(m, s), S.X[m * slots + s, 0:SEQ, :], 0.0)
        S.vimg[m] = S.vdx[m].astype(bf)
        for s in range(slots):
            S.vdx[m, :, s, :] = S.DX[m * slots + s, 0:SEQ, :]
        return c

    run(due(3.2))
    lax.fori_loop(0, NI // slots, out_tokens, 0)
    outs = [pltpu.make_async_copy(S.vimg, act, S.lsem.at[1]), pltpu.make_async_copy(S.vdx, dimg, S.lsem.at[2])]
    for out in outs:
        out.start()
    for l in range(1, L):
        total(l)
    rest = []
    while queue:
        rest += due(0.5)
    run(rest)
    total(0)
    outs.append(pltpu.make_async_copy(S.vm, o_grad, S.lsem.at[0]))
    outs[-1].start()
    for out in outs:
        out.wait()


NAMES = (
    ["Wq", "Wp", "Wu", "Wd", "V", "VG", "F", "X", "DX", "DO", "DM", "DA", "DQKV", "wgs"]
    + [name for name, _, _ in SAVED]
    + ["rb0"]
    + ["rb%d_%d" % (stage, c) for c in range(PARTS) for stage in (1, 2, 3)]
    + ["vm", "vimg", "vcot", "vdx"]
    + ["lsem", "gsend", "grecv", "rsend", "rr0", "rr1", "rr2", "rr3"]
)


def body(topo, images, cotangent, counts, master, moment_one, moment_two):
    micro, slots = images.shape[:2]
    NI = micro * slots
    L, width = master.shape
    rows = width // 128
    RP = 16 * ((rows + 15) // 16)
    nd = lax.axis_size("fsdp")
    (nz, _), (n1, _), (n2, _), (nc, _) = topo
    cut = parts(RP)

    VM, DMA = pltpu.VMEM, pltpu.SemaphoreType.DMA
    scratch = [
        VM((L, D, 3 * D), bf),
        VM((L, D, D), bf),
        VM((L, D, FF), bf),
        VM((L, FF, D), bf),
        VM((L, 16, FF), f32),
        VM((16, FF), f32),
        VM((nd * rows, 128), f32),
        VM((NI, TP, D), f32),
        VM((NI, TP, D), f32),
        VM((QP, D), bf),
        VM((NI, TP, D), bf),
        VM((NI, TP, D), bf),
        VM((NI, TP, 3 * D), bf),
        VM((L, nd, RP, 128), bf),
    ]
    scratch += [VM((L, NI) + shape, kind) for _, shape, kind in SAVED]
    scratch += [VM((L, max(nc - 1, 1), nz * n1 * n2, RP, 128), bf)]
    for c in range(PARTS):
        near, far = ((n2, n1), (n1, n2))[c % 2]
        scratch += [
            VM((L, max(near - 1, 1), nz * far, cut[c][1], 128), bf),
            VM((L, max(far - 1, 1), nz, cut[c][1], 128), bf),
            VM((L, max(nz - 1, 1), cut[c][1], 128), bf),
        ]
    tokens = (micro, SEQ, slots, D)
    scratch += [VM((rows, L, 128), f32), VM(tokens, bf), VM(tokens, bf), VM(tokens, f32)]
    wide_first = max(n1, n2, 2) - 1
    scratch += [
        DMA((3,)),
        DMA((L,)),
        DMA((L, PARTS, nd)),
        DMA((L,)),
        DMA((L, max(nc - 1, 1), nz * n1 * n2)),
        DMA((L, PARTS, wide_first, nz * max(n1, n2))),
        DMA((L, PARTS, wide_first, nz)),
        DMA((L, PARTS, max(nz - 1, 1))),
    ]
    anywhere = pl.BlockSpec(memory_space=pl.ANY)
    act, grad_in, grad = pl.pallas_call(
        functools.partial(kernel, (topo, L, NI, nd, rows, slots)),
        out_shape=(
            jax.ShapeDtypeStruct(tokens, bf),
            jax.ShapeDtypeStruct(tokens, f32),
            jax.ShapeDtypeStruct((rows, L, 128), f32),
        ),
        in_specs=[pl.BlockSpec(memory_space=pltpu.SMEM)] + [anywhere] * 3,
        out_specs=(anywhere,) * 3,
        scratch_shapes=scratch,
        compiler_params=pltpu.CompilerParams(vmem_limit_bytes=67043328, collective_id=0, has_side_effects=True),
        name="step",
    )(
        counts.T,
        images.transpose(0, 2, 1, 3),
        cotangent.transpose(0, 2, 1, 3),
        master.reshape(L, rows, 128).transpose(1, 0, 2),
    )
    weight_grad = grad.transpose(1, 0, 2).reshape(L, width) / (NI * nd)
    first_new = beta_one * moment_one + (1.0 - beta_one) * weight_grad
    second_new = beta_two * moment_two + (1.0 - beta_two) * weight_grad * weight_grad
    update = first_new / (1.0 - beta_one**STEP) / (jnp.sqrt(second_new / (1.0 - beta_two**STEP)) + epsilon)
    new_master = master - learn_rate * (update + decay_rate * master)
    return (
        act.transpose(0, 2, 1, 3),
        grad_in.transpose(0, 2, 1, 3),
        weight_grad,
        new_master,
        first_new,
        second_new,
    )


def solution(mesh):
    topo = topology(mesh)
    tokens = P(None, "fsdp", None, None)
    state = P(None, "fsdp")
    return jax.shard_map(
        functools.partial(body, topo),
        mesh=mesh,
        in_specs=(tokens, tokens, state, state, state, state),
        out_specs=(tokens, tokens, state, state, state, state),
        check_vma=False,
    )
```
